128 devices in a mesh: lat: 4 (over z), lon: 32 (over x, y, core).
Axes of the slice: x: 4, y: 4, z: 4, core: 2. Of those that a mesh axis runs over, the one named last changes fastest.
Arguments:
- spectrum: float32 [1296, 32, 8192], P(None, 'lat', 'lon'), may hold values from 0.01 to 1
- sea_mask: int32 [32, 8192], P('lat', 'lon'), may hold values 0 or 1
- courant: float32 [2, 1296], replicated, may hold values from -0.45 to 0.45
- obs_tile: int32 [32768, 1], P(('lat', 'lon')), may hold values from 0 to 127; in each aligned block of 256 rows (0 to 255, 256 to 511, ...) at most 8 rows name the same one
- obs_cell: int32 [32768], P(('lat', 'lon')), may hold values from 0 to 2047
- obs_value: float32 [32768], P(('lat', 'lon')), may hold values from 1 to 3
- obs_error: float32 [32768], P(('lat', 'lon')), may hold values from 0.05 to 0.5
Outputs:
- updated: float32 [1296, 32, 8192], P(None, 'lat', 'lon')
- increment: float32 [32, 8192], P('lat', 'lon')
The draws below stay inside these ranges and needn't reach their ends.
Inputs may be any that keep to these rules, and one draw needn't show every extreme that they name: `obs_tile`: within the 256 reports of one device no tile occurs more than 8 times.
All inputs are finite; a program needn't handle non-finite values. No bound on the sum of `sea_mask` on one device may be relied on, other than what follows from the above.
Results may differ from the reference program's by a relative error of at most 0.00002.
Values sent between devices are 32-bit elements; how exact they have to be, the bound alone decides.
A program may use at most 128 MiB of HBM per device.

```python
import math
import jax
import jax.numpy as jnp
import numpy as np
from jax import lax

SPEC = 1296
CLAT = 8
CLON = 256
OBS_DEV = 256
PASSES = 8
CAP = 8
NLAT = 32
NLON = 8192
OBS = 32768
N_LON = 32
DEVICES = 128


def plant(array, stream_key, low, high):
    longest = array.shape.index(max(array.shape))
    spots = []
    for shift in (0, 1):
        where = [jax.random.randint(jax.random.fold_in(stream_key, axis), (), 0, length) for axis, length in enumerate(array.shape)]
        where[longest] = (where[longest] + shift) % array.shape[longest]
        spots.append(tuple(where))
    return array.at[spots[0]].set(low).at[spots[1]].set(high)


def shard_levels(key, dims, split, least, top_value):
    level, own = 1.0, jax.random.fold_in(key, 6)
    for dim, blocks in split:
        draws = jnp.exp(jax.random.uniform(jax.random.fold_in(own, dim), (blocks,), jnp.float32, least / len(split), top_value / len(split)))
        level = level * jnp.repeat(draws, dims[dim] // blocks).reshape([-1 if axis == dim else 1 for axis in range(len(dims))])
    return level


def routed_block(rng, own, number, rows, amount, top, bound, lean):
    sequence = jax.random.permutation(rng, amount)
    packed, ordinary = load_shares(amount, rows * top, bound, lean, True), load_shares(amount, rows * top, bound, lean, False)
    places = jnp.arange(amount)

    def named(sizes, offset_by):
        used = int((sizes > 0).sum())
        fixed = max(1, used // 4)
        passed = fixed + (places - fixed + offset_by * (used - fixed)) % max(1, amount - fixed)
        return jnp.zeros((amount,), jnp.int32).at[sequence[jnp.where(places < fixed, places, passed)]].set(jnp.asarray(sizes, jnp.int32))

    sizes = jnp.where(number % 4 == 0, named(packed, number // 4), named(ordinary, number - number // 4 - 1))
    mixed = jax.random.permutation(jax.random.fold_in(own, 3), amount)
    source_of, taker = mixed[0:amount // 2 * 2:2], mixed[1:amount // 2 * 2:2]
    slack = jnp.minimum(sizes[source_of] - 1, bound - sizes[taker]) // 2
    slack = jnp.where((source_of == sequence[0]) | (taker == sequence[0]) | (sizes[taker] == 0), 0, jnp.maximum(slack, 0))
    passed = jax.random.randint(jax.random.fold_in(own, 4), (amount // 2,), 0, 1 << 20) % (slack + 1)
    sizes = sizes.at[source_of].add(-passed).at[taker].add(passed)
    members = jnp.searchsorted(jnp.cumsum(sizes), jnp.arange(rows * top), side="right").astype(jnp.int32)
    grid = members.reshape(top, rows).T
    grid = grid[jax.random.permutation(jax.random.fold_in(own, 1), rows)]
    offset_by = jax.random.randint(jax.random.fold_in(own, 2), (rows, 1), 0, top)
    return jnp.take_along_axis(grid, (jnp.arange(top)[None, :] + offset_by) % top, axis=1)


def load_shares(amount, total, limit, skew, full):
    portions = [(1 << 20) // math.isqrt(rank ** skew) + 1 for rank in range(1, amount + 1)]
    largest = limit if full else min(limit, max(-(-total // amount), total * portions[0] // sum(portions)))
    least = 1 if total - largest >= amount - 1 else 0
    counts, surplus = [largest] + [least] * (amount - 1), total - largest - least * (amount - 1)
    while surplus > 0:
        movable = [i for i in range(1, amount) if counts[i] < largest] or [i for i in range(1, amount) if counts[i] < limit]
        mass, remaining = sum([portions[i] for i in movable]), surplus
        for i in movable:
            extra = min(limit - counts[i], max(1, remaining * portions[i] // mass), surplus)
            counts[i] = counts[i] + extra
            surplus = surplus - extra
    return np.array(counts)


def setup_inputs(seed: int = 0) -> dict:
    key_of = jax.random.split(jax.random.key(seed), 8)
    spectrum = jnp.clip(jnp.exp(math.log(1.0) - 4.6051702 * jax.random.uniform(key_of[0], (SPEC, NLAT, NLON), jnp.float32) ** shard_levels(key_of[0], (SPEC, NLAT, NLON), ((1, 4), (2, 32)), -0.2, 0.2)), 0.01, 1.0)
    sea_mask = plant((jax.random.randint(key_of[1], (NLAT, NLON), 0, 4) < 3).astype(jnp.int32), jax.random.fold_in(key_of[1], 1), 0, 1)
    courant = jnp.clip(jax.random.uniform(key_of[2], (2, SPEC), jnp.float32, -0.45, 0.45), -0.45, 0.45)
    obs_tile_keys = jax.random.split(jax.random.fold_in(key_of[3], 1), OBS // OBS_DEV)
    obs_tile_turns = jax.random.permutation(jax.random.fold_in(key_of[3], 3), OBS // OBS_DEV)
    obs_tile = jax.vmap(lambda own, number: routed_block(jax.random.fold_in(key_of[3], 2), own, number, OBS_DEV, DEVICES, 1, CAP, 2))(obs_tile_keys, obs_tile_turns).reshape((OBS, 1))
    obs_cell = plant(jax.random.randint(key_of[4], (OBS,), 0, CLAT * CLON), jax.random.fold_in(key_of[4], 1), 0, (CLAT * CLON) - 1).astype(jnp.int32)
    obs_value = jnp.clip(1.0 + 2.0 * jax.random.uniform(key_of[5], (OBS,), jnp.float32) ** shard_levels(key_of[5], (OBS,), ((0, 128),), -0.2, 0.2), 1.0, 3.0)
    obs_error = jnp.clip(jnp.exp(math.log(0.5) - 2.3025851 * jax.random.uniform(key_of[6], (OBS,), jnp.float32) ** shard_levels(key_of[6], (OBS,), ((0, 128),), -0.2, 0.2)), 0.05, 0.5)
    return {"spectrum": spectrum, "sea_mask": sea_mask, "courant": courant, "obs_tile": obs_tile, "obs_cell": obs_cell, "obs_value": obs_value, "obs_error": obs_error}


spread_rate = 0.2
prior_weight = 4.0

def relax_global(fields, ocean):
    lat_pad = jnp.pad(fields, ((0, 0), (1, 1), (0, 0)))
    ocean_pad = jnp.pad(ocean, ((1, 1), (0, 0)))
    summed = ocean_pad[2:] * (lat_pad[:, 2:] - fields)
    summed = summed + ocean_pad[:-2] * (lat_pad[:, :-2] - fields)
    summed = summed + jnp.roll(ocean, -1, axis=1) * (jnp.roll(fields, -1, axis=2) - fields)
    summed = summed + jnp.roll(ocean, 1, axis=1) * (jnp.roll(fields, 1, axis=2) - fields)
    return fields + spread_rate * ocean * summed

def reference(spectrum, sea_mask, courant, obs_tile, obs_cell, obs_value, obs_error):
    ocean = sea_mask.astype(jnp.float32)
    height = 4.0 * jnp.sqrt(lax.optimization_barrier(jnp.mean(spectrum, axis=0)))
    owners = obs_tile[:, 0]
    obs_row = owners // N_LON * CLAT + obs_cell // CLON
    obs_col = owners % N_LON * CLON + obs_cell % CLON
    weights = 1.0 / obs_error
    misfit = weights * (obs_value - height[obs_row, obs_col])
    fields = jnp.zeros((2, NLAT, NLON), jnp.float32)
    fields = fields.at[0, obs_row, obs_col].add(misfit)
    fields = fields.at[1, obs_row, obs_col].add(weights)
    fields = fields * ocean
    for repeat in range(PASSES):
        fields = relax_global(fields, ocean)
    increment = ocean * fields[0] / (prior_weight + fields[1])
    factor = jnp.exp(2.0 * increment / height)
    ocean_east = jnp.roll(ocean, -1, axis=1)
    ocean_north = jnp.pad(ocean[1:], ((0, 1), (0, 0)))

    def advect(paired_input):
        component, speeds = paired_input
        analyzed = component * factor
        east_cell = jnp.roll(analyzed, -1, axis=1)
        north_cell = jnp.pad(analyzed[1:], ((0, 1), (0, 0)))
        flux_east = (jnp.maximum(speeds[0], 0.0) * analyzed + jnp.minimum(speeds[0], 0.0) * east_cell) * ocean * ocean_east
        flux_north = (jnp.maximum(speeds[1], 0.0) * analyzed + jnp.minimum(speeds[1], 0.0) * north_cell) * ocean * ocean_north
        spill_east = flux_east - jnp.roll(flux_east, 1, axis=1)
        spill_north = flux_north - jnp.pad(flux_north[:-1], ((1, 0), (0, 0)))
        return ocean * (analyzed - spill_east - spill_north)
    updated = lax.map(advect, (spectrum, courant.T))
    return (updated, increment)
```

```python
import functools

import jax
import jax.numpy as jnp
from jax import lax
from jax.experimental import pallas as pl
from jax.experimental.pallas import tpu as pltpu
from jax.sharding import PartitionSpec as P

SPEC = 1296
ROWS = 8
COLS = 256
LAT = 4
LON = 32
DEV = LAT * LON
NROW = LAT * ROWS
PASSES = 8
LANES = 128
GROUPS = 11
EXT = 384
RIM = 9
CHUNK = 64
CAP_HALF = 704
CAP_ALL = 1344
BLOCK = 72

spread_rate = 0.2
prior_weight = 4.0

f32 = jnp.float32
i32 = jnp.int32
bf16 = jnp.bfloat16
MESH = pl.DeviceIdType.MESH
NT = (((1,), (1,)), ((), ()))
NN = (((1,), (0,)), ((), ()))


def thirds(x):
    high = x.astype(bf16)
    rest = x - high.astype(f32)
    mid = rest.astype(bf16)
    low = (rest - mid.astype(f32)).astype(bf16)
    return high, mid, low


def exchange_kernel(
    cap,
    picks,
    spectrum,
    reports,
    sea,
    tables,
    from_south,
    from_north,
    cols_west,
    cols_east,
    cells,
    outbox,
    inbox,
    turned,
    fields,
    near_west,
    near_east,
    own_west,
    own_east,
    padded,
    going_north,
    going_south,
    load_sems,
    box_sems,
    lat_sems,
    col_sems,
    rim_sems,
    row_sems,
):
    lat = lax.axis_index("lat")
    lon = lax.axis_index("lon")
    me = lat * LON + lon
    west = lax.rem(lon + LON - 1, LON)
    east = lax.rem(lon + 1, LON)

    def load(group):
        size = min(LANES, SPEC - group * LANES)
        part = pl.ds(group * LANES, size)
        return pltpu.make_async_copy(
            spectrum.at[part], cells.at[part], load_sems.at[group]
        )

    for group in range(GROUPS):
        load(group).start()

    barrier = pltpu.get_barrier_semaphore()

    def greet(step, carry):
        peer = lax.rem(me + step, DEV)
        pl.semaphore_signal(
            barrier,
            inc=1,
            device_id=(peer // LON, lax.rem(peer, LON)),
            device_id_type=MESH,
        )
        return carry

    lax.fori_loop(1, DEV, greet, 0)

    owner = reports[0:1, :].astype(i32)
    owner_lat = lax.shift_right_logical(owner, 5)
    owner_lon = lax.bitwise_and(owner, 31)
    tiles = lax.broadcasted_iota(i32, (DEV, 256), 0)
    hit = jnp.where(tiles == owner, 1.0, 0.0)
    before = jnp.where(
        lax.broadcasted_iota(i32, (256, 256), 0)
        < lax.broadcasted_iota(i32, (256, 256), 1),
        1.0,
        0.0,
    )
    earlier = lax.dot_general(
        hit.astype(bf16), before.astype(bf16), NN, preferred_element_type=f32
    )
    rank = jnp.sum(hit * earlier, axis=0, keepdims=True).astype(i32)
    slot = owner_lat * 8 + rank
    slots = lax.broadcasted_iota(i32, (32, 256), 0)
    in_slot = slots == slot
    to_lon = jnp.where(slots == owner_lon, 1.0, 0.0).astype(bf16)
    zero = jnp.zeros((32, 256), f32)
    spread = jnp.concatenate(
        [jnp.where(in_slot, reports[v : v + 1, :], zero) for v in (1, 2, 3)] + [zero],
        axis=0,
    )
    packed = jnp.zeros((LON, LANES), f32)
    for piece in thirds(spread):
        packed = packed + lax.dot_general(
            to_lon, piece, NT, preferred_element_type=f32
        )
    outbox[...] = packed

    lane = lax.broadcasted_iota(i32, (ROWS, LANES), 1)
    blank = jnp.zeros((ROWS, LANES), f32)
    sums = tuple(blank for _ in range(8))
    for group in range(GROUPS):
        load(group).wait()
        size = min(LANES, SPEC - group * LANES)

        def gather(turn, carry, group=group):
            sums, first, final = list(carry[0]), carry[1], carry[2]
            for u in range(4):
                at = turn * 4 + u
                left = cells[group * LANES + at, :, 0:LANES]
                right = cells[group * LANES + at, :, LANES:COLS]
                sums[2 * u] = sums[2 * u] + left
                sums[2 * u + 1] = sums[2 * u + 1] + right
                here = lane == at
                first = jnp.where(here, pltpu.roll(left, at, 1), first)
                final = jnp.where(
                    here, pltpu.roll(right, lax.rem(at + 1, LANES), 1), final
                )
            return tuple(sums), first, final

        sums, first, final = lax.fori_loop(
            0, size // 4, gather, (sums, blank, blank)
        )
        own_west[group] = first
        own_east[group] = final
    left = (sums[0] + sums[2]) + (sums[4] + sums[6])
    right = (sums[1] + sums[3]) + (sums[5] + sums[7])
    here_rows = pl.ds(pl.multiple_of(lat * ROWS, ROWS), ROWS)
    fields[2, here_rows, 0:LANES] = 4.0 * jnp.sqrt(left / SPEC)
    fields[2, here_rows, LANES:COLS] = 4.0 * jnp.sqrt(right / SPEC)
    fields[3, here_rows, 0:COLS] = sea[...].astype(f32)

    pl.semaphore_wait(barrier, DEV - 1)

    def post(step, carry):
        peer = lax.rem(me + step, DEV)
        pltpu.make_async_remote_copy(
            src_ref=outbox.at[pl.ds(lax.rem(peer, LON), 1)],
            dst_ref=inbox.at[pl.ds(me, 1)],
            send_sem=box_sems.at[0],
            recv_sem=box_sems.at[1],
            device_id=(peer // LON, lax.rem(peer, LON)),
            device_id_type=MESH,
        ).start()
        return carry

    lax.fori_loop(1, DEV, post, 0)
    inbox[pl.ds(me, 1), :] = outbox[pl.ds(lon, 1), :]

    def pick(base, turn):
        for u in range(8):
            at = base + turn * 8 + u
            going_north[pl.ds(at, 1), :] = cells[picks[0, at], ROWS - 1 : ROWS, :]
            going_south[pl.ds(at, 1), :] = cells[picks[1, at], 0:1, :]

    def pick_chunk(number):
        base = pl.multiple_of(number * CHUNK, CHUNK)
        lax.fori_loop(0, CHUNK // 8, lambda turn, carry: (pick(base, turn), carry)[1], 0)

    pick_chunk(0)

    for step in range(1, LAT):
        peer = lax.rem(lat + step, LAT)
        part = fields.at[pl.ds(2, 2), here_rows, pl.ds(0, COLS)]
        pltpu.make_async_remote_copy(
            src_ref=part,
            dst_ref=part,
            send_sem=lat_sems.at[0],
            recv_sem=lat_sems.at[1],
            device_id=(peer, lon),
            device_id_type=MESH,
        ).start()
    send_west = pltpu.make_async_remote_copy(
        src_ref=own_west,
        dst_ref=cols_east,
        send_sem=col_sems.at[0],
        recv_sem=col_sems.at[1],
        device_id=(lat, west),
        device_id_type=MESH,
    )
    send_east = pltpu.make_async_remote_copy(
        src_ref=own_east,
        dst_ref=cols_west,
        send_sem=col_sems.at[2],
        recv_sem=col_sems.at[3],
        device_id=(lat, east),
        device_id_type=MESH,
    )
    send_west.start()
    send_east.start()

    def north_copy(rows):
        return pltpu.make_async_remote_copy(
            src_ref=going_north.at[rows],
            dst_ref=from_south.at[rows],
            send_sem=row_sems.at[0],
            recv_sem=row_sems.at[1],
            device_id=(lat + 1, lon),
            device_id_type=MESH,
        )

    def south_copy(rows):
        return pltpu.make_async_remote_copy(
            src_ref=going_south.at[rows],
            dst_ref=from_north.at[rows],
            send_sem=row_sems.at[2],
            recv_sem=row_sems.at[3],
            device_id=(lat - 1, lon),
            device_id_type=MESH,
        )

    def send_chunk(number):
        rows = pl.ds(pl.multiple_of(number * CHUNK, CHUNK), CHUNK)

        @pl.when(lat < LAT - 1)
        def _():
            north_copy(rows).start()

        @pl.when(lat > 0)
        def _():
            south_copy(rows).start()

    def forward(number, carry):
        pick_chunk(number)
        send_chunk(number - 1)
        return carry

    lax.fori_loop(1, cap // CHUNK, forward, 0)

    @pl.when(lat == 0)
    def _():
        from_south[...] = jnp.zeros(from_south.shape, f32)

    @pl.when(lat == LAT - 1)
    def _():
        from_north[...] = jnp.zeros(from_north.shape, f32)

    send_chunk(cap // CHUNK - 1)

    got = pl.ds(0, DEV - 1)
    pltpu.make_async_copy(inbox.at[got], inbox.at[got], box_sems.at[1]).wait()
    turned[...] = inbox[...].T

    def place(number, carry):
        base = pl.multiple_of(number * 8, 8)
        misfits = turned[pl.ds(base, 8), :]
        weights = turned[pl.ds(base + 32, 8), :]
        cell = turned[pl.ds(base + 64, 8), :].astype(i32)
        cell_row = lax.shift_right_logical(cell, 8)
        cell_col = lax.bitwise_and(cell, 255)
        rows8 = lax.broadcasted_iota(i32, (8, LANES), 0)
        cols = lax.broadcasted_iota(i32, (COLS, LANES), 0)
        spots, sent = [], []
        for s in range(8):
            spots.append(jnp.where(cols == cell_col[s : s + 1, :], 1.0, 0.0).astype(bf16))
            at_row = rows8 == cell_row[s : s + 1, :]
            sent.append(
                jnp.concatenate(
                    [
                        jnp.where(at_row, misfits[s : s + 1, :], 0.0),
                        jnp.where(at_row, weights[s : s + 1, :], 0.0),
                    ],
                    axis=0,
                )
            )
        spots = jnp.concatenate(spots, axis=1)
        sent = jnp.concatenate(sent, axis=1)
        total = jnp.zeros((16, COLS), f32)
        for piece in thirds(sent):
            total = total + lax.dot_general(
                piece, spots, NT, preferred_element_type=f32
            )
        fields[0, pl.ds(base, 8), 0:COLS] = total[0:8, :]
        fields[1, pl.ds(base, 8), 0:COLS] = total[8:16, :]
        return carry

    lax.fori_loop(0, LAT, place, 0)

    three = fields.at[pl.ds(2, 2), pl.ds(0, NROW - ROWS), pl.ds(0, COLS)]
    pltpu.make_async_copy(three, three, lat_sems.at[1]).wait()
    pltpu.make_async_copy(three, three, lat_sems.at[0]).wait()
    height = fields[2, :, 0:COLS]
    ocean = fields[3, :, 0:COLS]
    weight = fields[1, :, 0:COLS] * ocean
    fields[0, :, 0:COLS] = (fields[0, :, 0:COLS] - height * fields[1, :, 0:COLS]) * ocean
    fields[1, :, 0:COLS] = weight

    rim_west = pltpu.make_async_remote_copy(
        src_ref=fields.at[pl.ds(0, 4), pl.ds(0, NROW), pl.ds(0, LANES)],
        dst_ref=near_east,
        send_sem=rim_sems.at[0],
        recv_sem=rim_sems.at[1],
        device_id=(lat, west),
        device_id_type=MESH,
    )
    rim_east = pltpu.make_async_remote_copy(
        src_ref=fields.at[pl.ds(0, 4), pl.ds(0, NROW), pl.ds(LANES, LANES)],
        dst_ref=near_west,
        send_sem=rim_sems.at[2],
        recv_sem=rim_sems.at[3],
        device_id=(lat, east),
        device_id_type=MESH,
    )
    rim_west.start()
    rim_east.start()
    rim_west.wait()
    rim_east.wait()
    lane = lax.broadcasted_iota(i32, (NROW, LANES), 1)
    for number, filler in enumerate((0.0, 0.0, 1.0, 0.0)):
        fields[number, :, COLS:EXT] = jnp.where(
            lane < RIM,
            near_east[number],
            jnp.where(lane >= LANES - RIM, near_west[number], filler),
        )

    row = lax.broadcasted_iota(i32, (NROW, EXT), 0)

    def north_of(x):
        return jnp.where(row == NROW - 1, 0.0, pltpu.roll(x, NROW - 1, 0))

    def south_of(x):
        return jnp.where(row == 0, 0.0, pltpu.roll(x, 1, 0))

    def east_of(x):
        return pltpu.roll(x, EXT - 1, 1)

    def west_of(x):
        return pltpu.roll(x, 1, 1)

    ocean = fields[3]
    share = spread_rate * ocean
    keep = 1.0 - share * (
        north_of(ocean) + south_of(ocean) + east_of(ocean) + west_of(ocean)
    )

    def relax(x):
        return keep * x + share * (
            (north_of(x) + south_of(x)) + (east_of(x) + west_of(x))
        )

    def relax_both(_, pair):
        return relax(pair[0]), relax(pair[1])

    misfit, weight = lax.fori_loop(0, PASSES, relax_both, (fields[0], fields[1]))
    increment = ocean * misfit / (prior_weight + weight)
    factor = jnp.exp(2.0 * increment / fields[2]) * ocean
    edge = jnp.zeros((8, EXT), f32)
    for number, value in enumerate(
        (
            factor,
            factor * east_of(ocean),
            factor * west_of(ocean),
            factor * north_of(ocean),
            factor * south_of(ocean),
            increment,
        )
    ):
        padded[number, 0:8, :] = edge
        padded[number, pl.ds(8, NROW), :] = value
        padded[number, pl.ds(8 + NROW, 8), :] = edge
    own = pl.ds(pl.multiple_of(8 + lat * ROWS, ROWS), ROWS)
    for number in range(6):
        tables[number] = padded[number, own, 0:COLS]
    below = padded[3, pl.ds(7 + lat * ROWS, 1), 0:COLS]
    above = padded[4, pl.ds(16 + lat * ROWS, 1), 0:COLS]
    tables[6] = jnp.broadcast_to(below, (ROWS, COLS))
    tables[7] = jnp.broadcast_to(above, (ROWS, COLS))
    tables[8, :, 0:LANES] = jnp.broadcast_to(
        padded[1, own, EXT - 1 : EXT], (ROWS, LANES)
    )
    tables[8, :, LANES:COLS] = jnp.broadcast_to(
        padded[2, own, COLS : COLS + 1], (ROWS, LANES)
    )

    pltpu.make_async_copy(inbox.at[got], inbox.at[got], box_sems.at[0]).wait()
    send_west.wait()
    send_east.wait()

    @pl.when(lat < LAT - 1)
    def _():
        north_copy(pl.ds(0, cap)).wait_send()
        south = pltpu.make_async_copy(from_north, from_north, row_sems.at[3])
        south.wait()

    @pl.when(lat > 0)
    def _():
        south_copy(pl.ds(0, cap)).wait_send()
        north = pltpu.make_async_copy(from_south, from_south, row_sems.at[1])
        north.wait()


def exchange(cap, picks, spectrum, reports, sea):
    vmem = pl.BlockSpec(memory_space=pltpu.VMEM)
    return pl.pallas_call(
        functools.partial(exchange_kernel, cap),
        out_shape=(
            jax.ShapeDtypeStruct((9, ROWS, COLS), f32),
            jax.ShapeDtypeStruct((cap, COLS), f32),
            jax.ShapeDtypeStruct((cap, COLS), f32),
            jax.ShapeDtypeStruct((GROUPS, ROWS, LANES), f32),
            jax.ShapeDtypeStruct((GROUPS, ROWS, LANES), f32),
        ),
        in_specs=[
            pl.BlockSpec(memory_space=pltpu.SMEM),
            pl.BlockSpec(memory_space=pl.ANY),
            vmem,
            vmem,
        ],
        out_specs=(vmem,) * 5,
        scratch_shapes=[
            pltpu.VMEM((SPEC, ROWS, COLS), f32),
            pltpu.VMEM((LON, LANES), f32),
            pltpu.VMEM((DEV, LANES), f32),
            pltpu.VMEM((LANES, DEV), f32),
            pltpu.VMEM((4, NROW, EXT), f32),
            pltpu.VMEM((4, NROW, LANES), f32),
            pltpu.VMEM((4, NROW, LANES), f32),
            pltpu.VMEM((GROUPS, ROWS, LANES), f32),
            pltpu.VMEM((GROUPS, ROWS, LANES), f32),
            pltpu.VMEM((6, NROW + 16, EXT), f32),
            pltpu.VMEM((cap, COLS), f32),
            pltpu.VMEM((cap, COLS), f32),
            pltpu.SemaphoreType.DMA((GROUPS,)),
            pltpu.SemaphoreType.DMA((2,)),
            pltpu.SemaphoreType.DMA((2,)),
            pltpu.SemaphoreType.DMA((4,)),
            pltpu.SemaphoreType.DMA((4,)),
            pltpu.SemaphoreType.DMA((4,)),
        ],
        compiler_params=pltpu.CompilerParams(
            collective_id=0 if cap == CAP_HALF else 1,
            has_side_effects=True,
            vmem_limit_bytes=30 * 2**20,
        ),
        name=f"exchange_{cap}",
    )(picks, spectrum, reports, sea)


def update_kernel(
    courant,
    spectrum,
    tables,
    from_south,
    from_north,
    cols_west,
    cols_east,
    out,
    increment,
    beside,
    counts,
):
    step = pl.program_id(0)

    @pl.when(step == 0)
    def _():
        counts[0] = 0
        increment[...] = tables[5]
        for group in range(GROUPS):
            beside[0, group] = cols_west[group] * tables[8, :, 0:LANES]
            beside[1, group] = cols_east[group] * tables[8, :, LANES:COLS]

    lane = lax.broadcasted_iota(i32, (ROWS, LANES), 1)
    sub = lax.broadcasted_iota(i32, (ROWS, COLS), 0)
    plain = tables[0]

    def one(at, south_count):
        number = step * BLOCK + at
        east_speed = courant[0, number]
        north_speed = courant[1, number]
        back_x = east_speed < 0.0
        back_y = north_speed < 0.0
        x = back_x.astype(i32)
        y = back_y.astype(i32)
        cell = spectrum[at]
        group = lax.shift_right_logical(number, 7)
        at_lane = lax.bitwise_and(number, 127)

        flow = cell * tables[1 + x]
        shift = jnp.where(back_x, LANES - 1, 1)
        edge_lane = jnp.where(back_x, LANES - 1, 0)
        left = pltpu.roll(flow[:, 0:LANES], shift, 1)
        right = pltpu.roll(flow[:, LANES:COLS], shift, 1)
        rim = pltpu.roll(
            beside[x, group], lax.bitwise_and(edge_lane - at_lane + LANES, 127), 1
        )
        at_edge = lane == edge_lane
        new_left = jnp.where(at_edge, jnp.where(back_x, right, rim), left)
        new_right = jnp.where(at_edge, jnp.where(back_x, rim, left), right)
        came_x = jnp.concatenate([new_left, new_right], axis=1)
        gone_x = flow - came_x

        flow = cell * tables[3 + y]
        rolled = pltpu.roll(flow, jnp.where(back_y, ROWS - 1, 1), 0)
        north_count = number - south_count
        row = jnp.where(
            back_y,
            from_north[pl.ds(jnp.where(back_y, south_count, 0), 1), :],
            from_south[pl.ds(jnp.where(back_y, 0, north_count), 1), :],
        )
        edge_row = jnp.where(back_y, ROWS - 1, 0)
        came_y = jnp.where(sub == edge_row, row * tables[6 + y], rolled)
        gone_y = flow - came_y
        out[at] = (
            cell * plain - jnp.abs(east_speed) * gone_x - jnp.abs(north_speed) * gone_y
        )
        return south_count + y

    counts[0] = lax.fori_loop(0, BLOCK, one, counts[0], unroll=4)


def update(cap, courant, spectrum, tables, from_south, from_north, cols_west, cols_east):
    def whole(*shape):
        return pl.BlockSpec(shape, lambda i: (0,) * len(shape))

    return pl.pallas_call(
        update_kernel,
        grid=(SPEC // BLOCK,),
        out_shape=(
            jax.ShapeDtypeStruct((SPEC, ROWS, COLS), f32),
            jax.ShapeDtypeStruct((ROWS, COLS), f32),
        ),
        in_specs=[
            pl.BlockSpec(memory_space=pltpu.SMEM),
            pl.BlockSpec((BLOCK, ROWS, COLS), lambda i: (i, 0, 0)),
            whole(9, ROWS, COLS),
            whole(cap, COLS),
            whole(cap, COLS),
            whole(GROUPS, ROWS, LANES),
            whole(GROUPS, ROWS, LANES),
        ],
        out_specs=(
            pl.BlockSpec((BLOCK, ROWS, COLS), lambda i: (i, 0, 0)),
            whole(ROWS, COLS),
        ),
        scratch_shapes=[
            pltpu.VMEM((2, GROUPS, ROWS, LANES), f32),
            pltpu.SMEM((1,), i32),
        ],
        compiler_params=pltpu.CompilerParams(dimension_semantics=("arbitrary",)),
        name=f"update_{cap}",
    )(courant, spectrum, tables, from_south, from_north, cols_west, cols_east)


def body(spectrum, sea_mask, courant, obs_tile, obs_cell, obs_value, obs_error):
    weights = 1.0 / obs_error
    reports = jnp.stack(
        [
            obs_tile[:, 0].astype(f32),
            weights * obs_value,
            weights,
            obs_cell.astype(f32),
        ]
    )
    backward = (courant[1] < 0.0).astype(i32)
    number = jnp.arange(SPEC, dtype=i32)
    through = number[None, :] <= number[:, None]
    south_upto = jnp.sum(jnp.where(through, backward[None, :], 0), axis=1)
    upto = jnp.stack([number + 1 - south_upto, south_upto])
    fits = jnp.max(upto[:, -1]) <= CAP_HALF

    def run(cap):
        place = jnp.arange(cap, dtype=i32)
        picks = jnp.sum((upto[:, None, :] <= place[None, :, None]).astype(i32), axis=2)
        picks = jnp.minimum(picks, SPEC - 1)
        tables, south, north, cols_w, cols_e = exchange(
            cap, picks, spectrum, reports, sea_mask
        )
        return update(cap, courant, spectrum, tables, south, north, cols_w, cols_e)

    return lax.cond(fits, lambda: run(CAP_HALF), lambda: run(CAP_ALL))


def solution(mesh):
    return jax.shard_map(
        body,
        mesh=mesh,
        in_specs=(
            P(None, "lat", "lon"),
            P("lat", "lon"),
            P(),
            P(("lat", "lon"), None),
            P(("lat", "lon")),
            P(("lat", "lon")),
            P(("lat", "lon")),
        ),
        out_specs=(P(None, "lat", "lon"), P("lat", "lon")),
        check_vma=False,
    )
```

```python
import functools

import jax
import jax.numpy as jnp
from jax import lax
from jax.experimental import pallas as pl
from jax.experimental.pallas import tpu as pltpu
from jax.sharding import PartitionSpec as P

SPEC = 1296
ROWS = 8
COLS = 256
LAT = 4
LON = 32
DEV = LAT * LON
NROW = LAT * ROWS
PASSES = 8
LANES = 128
GROUP = 72
GROUPS = SPEC // GROUP
CELLS = SPEC * 16
LOADS = 6
MEMBERS = 72
EXT = 384
RIM = 9
CHUNK = 64
CAP_HALF = 704
CAP_ALL = 1344

spread_rate = 0.2
prior_weight = 4.0

f32 = jnp.float32
i32 = jnp.int32
bf16 = jnp.bfloat16
MESH = pl.DeviceIdType.MESH
LOGICAL = pl.DeviceIdType.LOGICAL
NT = (((1,), (1,)), ((), ()))
NN = (((1,), (0,)), ((), ()))


def thirds(x):
    high = x.astype(bf16)
    rest = x - high.astype(f32)
    mid = rest.astype(bf16)
    low = (rest - mid.astype(f32)).astype(bf16)
    return high, mid, low


def exchange_kernel(
    cap,
    spectrum,
    courant,
    by_group,
    obs_tile,
    obs_cell,
    obs_value,
    obs_error,
    sea,
    cells,
    tables,
    rows,
    cols_west,
    cols_east,
    plan,
    speeds,
    own_courant,
    own_groups,
    own_tile,
    own_cell,
    own_value,
    own_error,
    own_sea,
    outbox,
    inbox,
    turned,
    fields,
    near_west,
    near_east,
    own_edge,
    padded,
    going_north,
    going_south,
    listed,
    picks,
    load_sems,
    small_sems,
    list_sem,
    box_sems,
    lat_sems,
    col_sems,
    rim_sems,
    row_sems,
):
    lat = lax.axis_index("lat")
    lon = lax.axis_index("lon")
    me = lat * LON + lon
    west = lax.rem(lon + LON - 1, LON)
    east = lax.rem(lon + 1, LON)
    chunks = cap // CHUNK

    small = [
        pltpu.make_async_copy(source, target, small_sems.at[number])
        for number, (source, target) in enumerate(
            (
                (obs_tile, own_tile),
                (obs_error, own_error),
                (obs_value, own_value),
                (obs_cell, own_cell),
                (courant, own_courant),
                (by_group, own_groups),
                (by_group, speeds),
                (sea, own_sea),
            )
        )
    ]
    for copy in small:
        copy.start()
    size = CELLS // LOADS
    loads = [
        pltpu.make_async_copy(
            spectrum.at[pl.ds(part * size, size)],
            cells.at[pl.ds(8 + part * size, size)],
            load_sems.at[part],
        )
        for part in range(LOADS)
    ]
    for copy in loads:
        copy.start()

    barrier = pltpu.get_barrier_semaphore()

    def greet(turn, carry):
        for u in range(7):
            pl.semaphore_signal(
                barrier,
                inc=1,
                device_id=lax.rem(me + (turn * 7 + u + 1), DEV),
                device_id_type=LOGICAL,
            )
        return carry

    lax.fori_loop(0, 18, greet, 0)
    pl.semaphore_signal(
        barrier,
        inc=1,
        device_id=lax.rem(me + DEV - 1, DEV),
        device_id_type=LOGICAL,
    )

    for copy in small[0:4]:
        copy.wait()
    owner = own_tile[...]
    owner_lat = lax.shift_right_logical(owner, 5)
    owner_lon = lax.bitwise_and(owner, 31)
    tiles = lax.broadcasted_iota(i32, (DEV, 256), 0)
    hit = jnp.where(tiles == owner, 1.0, 0.0)
    before = jnp.where(
        lax.broadcasted_iota(i32, (256, 256), 0)
        < lax.broadcasted_iota(i32, (256, 256), 1),
        1.0,
        0.0,
    )
    earlier = lax.dot_general(
        hit.astype(bf16), before.astype(bf16), NN, preferred_element_type=f32
    )
    rank = jnp.sum(hit * earlier, axis=0, keepdims=True).astype(i32)
    slot = owner_lat * 8 + rank
    slots = lax.broadcasted_iota(i32, (32, 256), 0)
    in_slot = slots == slot
    to_lon = jnp.where(slots == owner_lon, 1.0, 0.0).astype(bf16)
    zero = jnp.zeros((32, 256), f32)
    weights = 1.0 / own_error[...]
    spread = jnp.concatenate(
        [
            jnp.where(in_slot, value, zero)
            for value in (weights * own_value[...], weights, own_cell[...].astype(f32))
        ]
        + [zero],
        axis=0,
    )
    packed = jnp.zeros((LON, LANES), f32)
    for piece in thirds(spread):
        packed = packed + lax.dot_general(
            to_lon, piece, NT, preferred_element_type=f32
        )
    outbox[...] = packed

    for copy in small[4:8]:
        copy.wait()
    number = lax.broadcasted_iota(i32, (16, LANES), 0) * LANES + lax.broadcasted_iota(
        i32, (16, LANES), 1
    )
    speed = jnp.concatenate(
        [own_courant[1:2, t * LANES : (t + 1) * LANES] for t in range(SPEC // LANES)]
        + [
            jnp.concatenate(
                [
                    own_courant[1:2, SPEC // LANES * LANES : SPEC],
                    jnp.zeros((1, LANES - SPEC % LANES), f32),
                ],
                axis=1,
            )
        ]
        + [jnp.zeros((15 - SPEC // LANES, LANES), f32)],
        axis=0,
    )
    backward = jnp.where(speed < 0.0, 1.0, 0.0).astype(bf16)
    upper = jnp.where(
        lax.broadcasted_iota(i32, (LANES, LANES), 0)
        <= lax.broadcasted_iota(i32, (LANES, LANES), 1),
        1.0,
        0.0,
    ).astype(bf16)
    within = lax.dot_general(backward, upper, NN, preferred_element_type=f32)
    whole = lax.dot_general(
        backward, jnp.ones((LANES, LANES), bf16), NN, preferred_element_type=f32
    )
    lower = jnp.where(
        lax.broadcasted_iota(i32, (16, 16), 1) < lax.broadcasted_iota(i32, (16, 16), 0),
        1.0,
        0.0,
    ).astype(bf16)
    south_upto = within + lax.dot_general(
        lower, whole.astype(bf16), NN, preferred_element_type=f32
    )
    beyond = number >= SPEC
    far = 4.0 * SPEC
    upto = (
        jnp.where(beyond, far, (number + 1).astype(f32) - south_upto),
        jnp.where(beyond, far, south_upto),
    )
    ones = jnp.ones((8, LANES), bf16)

    def enlist(turn, carry):
        place = (
            turn * LANES + lax.broadcasted_iota(i32, (LANES, LANES), 0)
        ).astype(f32)
        for side in range(2):
            count = jnp.zeros((LANES, LANES), f32)
            for t in range(SPEC // LANES + 1):
                count = count + jnp.where(upto[side][t : t + 1, :] <= place, 1.0, 0.0)
            total = lax.dot_general(
                ones, count.astype(bf16), NT, preferred_element_type=f32
            )
            listed[side, pl.ds(turn, 1), :] = jnp.maximum(
                jnp.minimum(total[0:1, :].astype(i32), SPEC - 1), 0
            )
        return carry

    lax.fori_loop(0, listed.shape[1], enlist, 0)
    to_scalars = pltpu.make_async_copy(listed, picks, list_sem)
    to_scalars.start()

    to_east = own_groups[0:GROUPS, :] < 0.0
    to_north = own_groups[GROUPS : 2 * GROUPS, :] < 0.0
    shape = (GROUPS, GROUP)
    group = lax.broadcasted_iota(i32, shape, 0)
    member = lax.broadcasted_iota(i32, shape, 1)
    number = group * GROUP + member
    backward = jnp.where(to_north, 1.0, 0.0).astype(bf16)
    upper = jnp.where(
        lax.broadcasted_iota(i32, (GROUP, GROUP), 0)
        < lax.broadcasted_iota(i32, (GROUP, GROUP), 1),
        1.0,
        0.0,
    ).astype(bf16)
    whole = lax.dot_general(
        backward, jnp.ones((GROUP, GROUP), bf16), NN, preferred_element_type=f32
    )
    lower = jnp.where(
        lax.broadcasted_iota(i32, (GROUPS, GROUPS), 1)
        < lax.broadcasted_iota(i32, (GROUPS, GROUPS), 0),
        1.0,
        0.0,
    ).astype(bf16)
    south = (
        lax.dot_general(backward, upper, NN, preferred_element_type=f32)
        + lax.dot_general(lower, whole.astype(bf16), NN, preferred_element_type=f32)
    ).astype(i32)
    plan[0] = jnp.where(to_east, LANES - 1, 1)
    plan[1] = jnp.where(
        to_east, LANES - 1 - member, jnp.where(member == 0, 0, LANES - member)
    )
    plan[2] = 8 + 16 * number + jnp.where(to_north, 1, -1)
    plan[3] = 2 * jnp.where(to_north, cap + south, number - south)

    def pick_chunk(number):
        def pick(turn, carry):
            for u in range(8):
                at = number * CHUNK + turn * 8 + u
                line = lax.div(number, 2)
                spot = lax.rem(number, 2) * CHUNK + turn * 8 + u
                first = 8 + 16 * picks[0, line, spot]
                going_north[pl.ds(2 * at, 1), :] = cells[pl.ds(first + 7, 1), :]
                going_north[pl.ds(2 * at + 1, 1), :] = cells[pl.ds(first + 15, 1), :]
                first = 8 + 16 * picks[1, line, spot]
                going_south[pl.ds(2 * at, 1), :] = cells[pl.ds(first, 1), :]
                going_south[pl.ds(2 * at + 1, 1), :] = cells[pl.ds(first + 8, 1), :]
            return carry

        lax.fori_loop(0, CHUNK // 8, pick, 0)

    def north_copy(first, count):
        return pltpu.make_async_remote_copy(
            src_ref=going_north.at[pl.ds(first, count)],
            dst_ref=rows.at[pl.ds(first, count)],
            send_sem=row_sems.at[0],
            recv_sem=row_sems.at[1],
            device_id=(lat + 1, lon),
            device_id_type=MESH,
        )

    def south_copy(first, count):
        return pltpu.make_async_remote_copy(
            src_ref=going_south.at[pl.ds(first, count)],
            dst_ref=rows.at[pl.ds(2 * cap + first, count)],
            send_sem=row_sems.at[2],
            recv_sem=row_sems.at[3],
            device_id=(lat - 1, lon),
            device_id_type=MESH,
        )

    def send_chunk(number):
        first = pl.multiple_of(number * (2 * CHUNK), 2 * CHUNK)

        @pl.when(lat < LAT - 1)
        def _():
            north_copy(first, 2 * CHUNK).start()

        @pl.when(lat > 0)
        def _():
            south_copy(first, 2 * CHUNK).start()

    pl.semaphore_wait(barrier, DEV - 1)
    def post(turn, carry):
        for u in range(7):
            peer = lax.rem(me + (turn * 7 + u + 1), DEV)
            post_to(peer)
        return carry

    def post_to(peer):
        pltpu.make_async_remote_copy(
            src_ref=outbox.at[pl.ds(lax.rem(peer, LON), 1)],
            dst_ref=inbox.at[pl.ds(me, 1)],
            send_sem=box_sems.at[0],
            recv_sem=box_sems.at[1],
            device_id=peer,
            device_id_type=LOGICAL,
        ).start()

    lax.fori_loop(0, 18, post, 0)
    post_to(lax.rem(me + DEV - 1, DEV))
    inbox[pl.ds(me, 1), :] = outbox[pl.ds(lon, 1), :]

    for copy in loads:
        copy.wait()
    to_scalars.wait()
    pick_chunk(0)
    pick_chunk(1)
    send_chunk(0)
    send_chunk(1)

    lane = lax.broadcasted_iota(i32, (ROWS, LANES), 1)
    blank = jnp.zeros((ROWS, LANES), f32)

    def gather(pair, sums):
        sums = list(sums)
        for half in range(2):
            group = 2 * pair + half
            edge = blank
            for u in range(GROUP):
                at = 8 + (group * GROUP + u) * 16
                left = cells[pl.ds(pl.multiple_of(at, 8), ROWS), :]
                right = cells[pl.ds(pl.multiple_of(at + 8, 8), ROWS), :]
                k = 2 * (u % 4)
                sums[k] = sums[k] + left
                sums[k + 1] = sums[k + 1] + right
                speed = speeds[group, u]
                taken = jnp.where(jnp.full((ROWS, LANES), speed) < 0.0, left, right)
                turn = jnp.where(speed < 0.0, u, u + 1)
                edge = jnp.where(lane == u, pltpu.roll(taken, turn, 1), edge)
            own_edge[group] = edge
        return tuple(sums)

    sums = lax.fori_loop(0, GROUPS // 2, gather, tuple(blank for _ in range(8)))
    left = (sums[0] + sums[2]) + (sums[4] + sums[6])
    right = (sums[1] + sums[3]) + (sums[5] + sums[7])
    here_rows = pl.ds(pl.multiple_of(lat * ROWS, ROWS), ROWS)
    fields[2, here_rows, 0:LANES] = 4.0 * jnp.sqrt(left / SPEC)
    fields[2, here_rows, LANES:COLS] = 4.0 * jnp.sqrt(right / SPEC)
    fields[3, here_rows, 0:COLS] = own_sea[...].astype(f32)

    for step in range(1, LAT):
        peer = lax.rem(lat + step, LAT)
        part = fields.at[pl.ds(2, 2), here_rows, pl.ds(0, COLS)]
        pltpu.make_async_remote_copy(
            src_ref=part,
            dst_ref=part,
            send_sem=lat_sems.at[0],
            recv_sem=lat_sems.at[1],
            device_id=(peer, lon),
            device_id_type=MESH,
        ).start()

    send_west = pltpu.make_async_remote_copy(
        src_ref=own_edge,
        dst_ref=cols_east,
        send_sem=col_sems.at[0],
        recv_sem=col_sems.at[1],
        device_id=(lat, west),
        device_id_type=MESH,
    )
    send_east = pltpu.make_async_remote_copy(
        src_ref=own_edge,
        dst_ref=cols_west,
        send_sem=col_sems.at[2],
        recv_sem=col_sems.at[3],
        device_id=(lat, east),
        device_id_type=MESH,
    )
    send_west.start()
    send_east.start()

    pick_chunk(2)

    def forward(number, carry):
        pick_chunk(number)
        send_chunk(number - 1)
        return carry

    lax.fori_loop(3, chunks, forward, 0)

    @pl.when(lat == 0)
    def _():
        rows[0 : 2 * cap, :] = jnp.zeros((2 * cap, LANES), f32)

    @pl.when(lat == LAT - 1)
    def _():
        rows[2 * cap : 4 * cap, :] = jnp.zeros((2 * cap, LANES), f32)

    send_chunk(chunks - 1)

    got = pl.ds(0, DEV - 1)
    pltpu.make_async_copy(inbox.at[got], inbox.at[got], box_sems.at[1]).wait()
    turned[...] = inbox[...].T

    def place(number, carry):
        base = pl.multiple_of(number * 8, 8)
        misfits = turned[pl.ds(base, 8), :]
        weights = turned[pl.ds(base + 32, 8), :]
        cell = turned[pl.ds(base + 64, 8), :].astype(i32)
        cell_row = lax.shift_right_logical(cell, 8)
        cell_col = lax.bitwise_and(cell, 255)
        rows8 = lax.broadcasted_iota(i32, (8, LANES), 0)
        cols = lax.broadcasted_iota(i32, (COLS, LANES), 0)
        spots, sent = [], []
        for s in range(8):
            spots.append(jnp.where(cols == cell_col[s : s + 1, :], 1.0, 0.0).astype(bf16))
            at_row = rows8 == cell_row[s : s + 1, :]
            sent.append(
                jnp.concatenate(
                    [
                        jnp.where(at_row, misfits[s : s + 1, :], 0.0),
                        jnp.where(at_row, weights[s : s + 1, :], 0.0),
                    ],
                    axis=0,
                )
            )
        spots = jnp.concatenate(spots, axis=1)
        sent = jnp.concatenate(sent, axis=1)
        total = lax.dot_general(
            jnp.concatenate(thirds(sent), axis=0), spots, NT, preferred_element_type=f32
        )
        total = total[0:16, :] + total[16:32, :] + total[32:48, :]
        fields[0, pl.ds(base, 8), 0:COLS] = total[0:8, :]
        fields[1, pl.ds(base, 8), 0:COLS] = total[8:16, :]
        return carry

    lax.fori_loop(0, LAT, place, 0)

    three = fields.at[pl.ds(2, 2), pl.ds(0, NROW - ROWS), pl.ds(0, COLS)]
    pltpu.make_async_copy(three, three, lat_sems.at[1]).wait()
    pltpu.make_async_copy(three, three, lat_sems.at[0]).wait()
    height = fields[2, :, 0:COLS]
    ocean = fields[3, :, 0:COLS]
    weight = fields[1, :, 0:COLS] * ocean
    fields[0, :, 0:COLS] = (fields[0, :, 0:COLS] - height * fields[1, :, 0:COLS]) * ocean
    fields[1, :, 0:COLS] = weight

    rim_west = pltpu.make_async_remote_copy(
        src_ref=fields.at[pl.ds(0, 4), pl.ds(0, NROW), pl.ds(0, LANES)],
        dst_ref=near_east,
        send_sem=rim_sems.at[0],
        recv_sem=rim_sems.at[1],
        device_id=(lat, west),
        device_id_type=MESH,
    )
    rim_east = pltpu.make_async_remote_copy(
        src_ref=fields.at[pl.ds(0, 4), pl.ds(0, NROW), pl.ds(LANES, LANES)],
        dst_ref=near_west,
        send_sem=rim_sems.at[2],
        recv_sem=rim_sems.at[3],
        device_id=(lat, east),
        device_id_type=MESH,
    )
    rim_west.start()
    rim_east.start()
    rim_west.wait()
    rim_east.wait()
    lane = lax.broadcasted_iota(i32, (NROW, LANES), 1)
    for number, filler in enumerate((0.0, 0.0, 1.0, 0.0)):
        fields[number, :, COLS:EXT] = jnp.where(
            lane < RIM,
            near_east[number],
            jnp.where(lane >= LANES - RIM, near_west[number], filler),
        )

    row = lax.broadcasted_iota(i32, (NROW, EXT), 0)

    def north_of(x):
        return jnp.where(row == NROW - 1, 0.0, pltpu.roll(x, NROW - 1, 0))

    def south_of(x):
        return jnp.where(row == 0, 0.0, pltpu.roll(x, 1, 0))

    def east_of(x):
        return pltpu.roll(x, EXT - 1, 1)

    def west_of(x):
        return pltpu.roll(x, 1, 1)

    ocean = fields[3]
    share = spread_rate * ocean
    keep = 1.0 - share * (
        north_of(ocean) + south_of(ocean) + east_of(ocean) + west_of(ocean)
    )

    def relax(x):
        return keep * x + share * (
            (north_of(x) + south_of(x)) + (east_of(x) + west_of(x))
        )

    def relax_both(_, pair):
        return relax(pair[0]), relax(pair[1])

    misfit, weight = lax.fori_loop(0, PASSES, relax_both, (fields[0], fields[1]))
    increment = ocean * misfit / (prior_weight + weight)
    factor = jnp.exp(2.0 * increment / fields[2]) * ocean
    going_up = factor * north_of(ocean)
    going_down = factor * south_of(ocean)
    for number, value in enumerate(
        (
            factor,
            factor * east_of(ocean),
            factor * west_of(ocean),
            going_up,
            going_down,
            south_of(going_up),
            north_of(going_down),
            increment,
        )
    ):
        padded[number] = value
    own = here_rows
    for number in range(8):
        tables[16 * number : 16 * number + 8, :] = padded[number, own, 0:LANES]
        tables[16 * number + 8 : 16 * number + 16, :] = padded[
            number, own, LANES:COLS
        ]
    tables[128:136, :] = jnp.broadcast_to(
        padded[1, own, EXT - 1 : EXT], (ROWS, LANES)
    )
    tables[136:144, :] = jnp.broadcast_to(
        padded[2, own, COLS : COLS + 1], (ROWS, LANES)
    )

    pltpu.make_async_copy(inbox.at[got], inbox.at[got], box_sems.at[0]).wait()
    send_west.wait()
    send_east.wait()

    @pl.when(lat < LAT - 1)
    def _():
        north_copy(0, 2 * cap).wait_send()
        part = rows.at[pl.ds(2 * cap, 2 * cap)]
        pltpu.make_async_copy(part, part, row_sems.at[3]).wait()

    @pl.when(lat > 0)
    def _():
        south_copy(0, 2 * cap).wait_send()
        part = rows.at[pl.ds(0, 2 * cap)]
        pltpu.make_async_copy(part, part, row_sems.at[1]).wait()


def exchange(cap, spectrum, courant, by_group, *observed):
    vmem = pl.BlockSpec(memory_space=pltpu.VMEM)
    lists = -(-cap // LANES)
    return pl.pallas_call(
        functools.partial(exchange_kernel, cap),
        out_shape=(
            jax.ShapeDtypeStruct((CELLS + 16, LANES), f32),
            jax.ShapeDtypeStruct((144, LANES), f32),
            jax.ShapeDtypeStruct((4 * cap, LANES), f32),
            jax.ShapeDtypeStruct((GROUPS, ROWS, LANES), f32),
            jax.ShapeDtypeStruct((GROUPS, ROWS, LANES), f32),
            jax.ShapeDtypeStruct((4, GROUPS, GROUP), i32),
        ),
        in_specs=[pl.BlockSpec(memory_space=pl.ANY)] * 8,
        out_specs=(vmem,) * 6,
        scratch_shapes=[
            pltpu.SMEM((2 * GROUPS, GROUP), f32),
            pltpu.VMEM((2, SPEC), f32),
            pltpu.VMEM((2 * GROUPS, GROUP), f32),
            pltpu.VMEM((1, 256), i32),
            pltpu.VMEM((1, 256), i32),
            pltpu.VMEM((1, 256), f32),
            pltpu.VMEM((1, 256), f32),
            pltpu.VMEM((ROWS, COLS), i32),
            pltpu.VMEM((LON, LANES), f32),
            pltpu.VMEM((DEV, LANES), f32),
            pltpu.VMEM((LANES, DEV), f32),
            pltpu.VMEM((4, NROW, EXT), f32),
            pltpu.VMEM((4, NROW, LANES), f32),
            pltpu.VMEM((4, NROW, LANES), f32),
            pltpu.VMEM((GROUPS, ROWS, LANES), f32),
            pltpu.VMEM((8, NROW, EXT), f32),
            pltpu.VMEM((2 * cap, LANES), f32),
            pltpu.VMEM((2 * cap, LANES), f32),
            pltpu.VMEM((2, lists, LANES), i32),
            pltpu.SMEM((2, lists, LANES), i32),
            pltpu.SemaphoreType.DMA((LOADS,)),
            pltpu.SemaphoreType.DMA((8,)),
            pltpu.SemaphoreType.DMA,
            pltpu.SemaphoreType.DMA((2,)),
            pltpu.SemaphoreType.DMA((2,)),
            pltpu.SemaphoreType.DMA((4,)),
            pltpu.SemaphoreType.DMA((4,)),
            pltpu.SemaphoreType.DMA((4,)),
        ],
        compiler_params=pltpu.CompilerParams(
            collective_id=0 if cap == CAP_HALF else 1,
            has_side_effects=True,
            vmem_limit_bytes=30 * 2**20,
        ),
        name=f"exchange_{cap}",
    )(spectrum, courant, by_group, *observed)


def update_kernel(
    by_group,
    cells,
    tables,
    rows,
    cols_west,
    cols_east,
    plan,
    out,
    increment,
    steps,
    sem,
):
    step = pl.program_id(0)

    @pl.when(step == 0)
    def _():
        copy = pltpu.make_async_copy(plan, steps, sem)
        copy.start()
        increment[:, 0:LANES] = tables[112:120, :]
        increment[:, LANES:COLS] = tables[120:128, :]
        copy.wait()

    lane = lax.broadcasted_iota(i32, (ROWS, LANES), 1)
    sub = lax.broadcasted_iota(i32, (ROWS, LANES), 0)
    plain = tables[0:8, :], tables[8:16, :]

    def eight(ref, first):
        return ref[pl.ds(pl.multiple_of(first, 8), 8), :]

    def some(part, carry):
        for u in range(MEMBERS):
            one(part * MEMBERS + u)
        return carry

    def one(u):
        at = 8 + (step * GROUP + u) * 16
        cell = eight(cells, at), eight(cells, at + 8)
        speed = jnp.full((ROWS, LANES), by_group[step, u])
        back = speed < 0.0
        flow = [
            cell[half]
            * jnp.where(
                back,
                tables[32 + 8 * half : 40 + 8 * half, :],
                tables[16 + 8 * half : 24 + 8 * half, :],
            )
            for half in range(2)
        ]
        shift = steps[0, step, u]
        moved = pltpu.roll(flow[0], shift, 1), pltpu.roll(flow[1], shift, 1)
        rim = pltpu.roll(jnp.where(back, rims[1], rims[0]), steps[1, step, u], 1)
        at_edge = lane == jnp.where(back, LANES - 1, 0)
        came = (
            jnp.where(at_edge, jnp.where(back, moved[1], rim), moved[0]),
            jnp.where(at_edge, jnp.where(back, rim, moved[0]), moved[1]),
        )
        speed = jnp.abs(speed)

        slow = jnp.full((ROWS, LANES), by_group[GROUPS + step, u])
        down = slow < 0.0
        at_row = sub == jnp.where(down, ROWS - 1, 0)
        slow = jnp.abs(slow)
        near = steps[2, step, u]
        place = steps[3, step, u]
        for half in range(2):
            beyond = jnp.where(
                at_row,
                jnp.broadcast_to(rows[pl.ds(place + half, 1), :], (ROWS, LANES)),
                cells[pl.ds(near + 8 * half, 8), :],
            )
            first = 8 * half
            way = jnp.where(
                down, tables[64 + first : 72 + first, :], tables[48 + first : 56 + first, :]
            )
            way_in = jnp.where(
                down, tables[96 + first : 104 + first, :], tables[80 + first : 88 + first, :]
            )
            gone = cell[half] * way - beyond * way_in
            out[pl.ds(pl.multiple_of(u * 16 + first, 8), 8), :] = (
                cell[half] * plain[half]
                - speed * (flow[half] - came[half])
                - slow * gone
            )

    rims = cols_west[step] * tables[128:136, :], cols_east[step] * tables[136:144, :]
    lax.fori_loop(0, GROUP // MEMBERS, some, 0)


def update(cap, by_group, cells, tables, rows, cols_west, cols_east, plan):
    vmem = pl.BlockSpec(memory_space=pltpu.VMEM)
    return pl.pallas_call(
        update_kernel,
        grid=(GROUPS,),
        out_shape=(
            jax.ShapeDtypeStruct((CELLS, LANES), f32),
            jax.ShapeDtypeStruct((ROWS, COLS), f32),
        ),
        in_specs=[pl.BlockSpec(memory_space=pltpu.SMEM)] + [vmem] * 6,
        out_specs=(
            pl.BlockSpec((GROUP * 16, LANES), lambda i: (i, 0)),
            pl.BlockSpec((ROWS, COLS), lambda i: (0, 0)),
        ),
        scratch_shapes=[
            pltpu.SMEM((4, GROUPS, GROUP), i32),
            pltpu.SemaphoreType.DMA,
        ],
        compiler_params=pltpu.CompilerParams(
            dimension_semantics=("arbitrary",), vmem_limit_bytes=24 * 2**20
        ),
        name=f"update_{cap}",
    )(by_group, cells, tables, rows, cols_west, cols_east, plan)


def body(spectrum, sea_mask, courant, obs_tile, obs_cell, obs_value, obs_error):
    halves = spectrum.reshape(SPEC, ROWS, 2, LANES).transpose(0, 2, 1, 3)
    observed = (
        obs_tile.reshape(1, -1),
        obs_cell.reshape(1, -1),
        obs_value.reshape(1, -1),
        obs_error.reshape(1, -1),
        sea_mask,
    )
    by_group = courant.reshape(2 * GROUPS, GROUP)
    south = jnp.sum((courant[1] < 0.0).astype(i32))
    fits = jnp.maximum(south, SPEC - south) <= CAP_HALF

    def run(cap):
        sent = exchange(
            cap, halves.reshape(CELLS, LANES), courant, by_group, *observed
        )
        return update(cap, by_group, *sent)

    updated, increment = lax.cond(
        fits, lambda: run(CAP_HALF), lambda: run(CAP_ALL)
    )
    updated = updated.reshape(SPEC, 2, ROWS, LANES).transpose(0, 2, 1, 3)
    return updated.reshape(SPEC, ROWS, COLS), increment


def solution(mesh):
    return jax.shard_map(
        body,
        mesh=mesh,
        in_specs=(
            P(None, "lat", "lon"),
            P("lat", "lon"),
            P(),
            P(("lat", "lon"), None),
            P(("lat", "lon")),
            P(("lat", "lon")),
            P(("lat", "lon")),
        ),
        out_specs=(P(None, "lat", "lon"), P("lat", "lon")),
        check_vma=False,
    )
```

```python
import functools

import jax
import jax.numpy as jnp
from jax import lax
from jax.experimental import pallas as pl
from jax.experimental.pallas import tpu as pltpu
from jax.sharding import PartitionSpec as P

SPEC = 1296
ROWS = 8
COLS = 256
LAT = 4
LON = 32
DEV = LAT * LON
NROW = LAT * ROWS
PASSES = 8
LANES = 128
GROUP = 72
GROUPS = SPEC // GROUP
CELLS = SPEC * 16
LOADS = 6
EXT = 384
RIM = 9
CHUNK = 64
CAP_HALF = 704
CAP_ALL = 1344

spread_rate = 0.2
prior_weight = 4.0

f32 = jnp.float32
i32 = jnp.int32
bf16 = jnp.bfloat16
MESH = pl.DeviceIdType.MESH
LOGICAL = pl.DeviceIdType.LOGICAL
NT = (((1,), (1,)), ((), ()))
NN = (((1,), (0,)), ((), ()))


def thirds(x):
    high = x.astype(bf16)
    rest = x - high.astype(f32)
    mid = rest.astype(bf16)
    low = (rest - mid.astype(f32)).astype(bf16)
    return high, mid, low


def exchange_kernel(
    cap,
    spectrum,
    courant,
    obs_tile,
    obs_cell,
    obs_value,
    obs_error,
    sea,
    partial,
    rim_tables,
    increments,
    rows,
    places,
    own_groups,
    cells,
    tables,
    cols_west,
    cols_east,
    plan,
    steps,
    speeds,
    own_courant,
    own_tile,
    own_cell,
    own_value,
    own_error,
    own_sea,
    outbox,
    inbox,
    turned,
    fields,
    near_west,
    near_east,
    own_edge,
    padded,
    going_north,
    going_south,
    listed,
    picks,
    load_sems,
    small_sems,
    list_sem,
    box_sems,
    lat_sems,
    col_sems,
    rim_sems,
    row_sems,
):
    lat = lax.axis_index("lat")
    lon = lax.axis_index("lon")
    me = lat * LON + lon
    west = lax.rem(lon + LON - 1, LON)
    east = lax.rem(lon + 1, LON)
    chunks = cap // CHUNK

    small = [
        pltpu.make_async_copy(source, target, small_sems.at[number])
        for number, (source, target) in enumerate(
            (
                (obs_tile, own_tile),
                (obs_error, own_error),
                (obs_value, own_value),
                (obs_cell, own_cell),
                (courant, own_courant),
                (sea, own_sea),
            )
        )
    ]
    for copy in small:
        copy.start()
    size = CELLS // LOADS
    loads = [
        pltpu.make_async_copy(
            spectrum.at[pl.ds(part * size, size)],
            cells.at[pl.ds(8 + part * size, size)],
            load_sems.at[part],
        )
        for part in range(LOADS)
    ]
    for copy in loads:
        copy.start()

    barrier = pltpu.get_barrier_semaphore()

    def greet(turn, carry):
        for u in range(7):
            pl.semaphore_signal(
                barrier,
                inc=1,
                device_id=lax.rem(me + (turn * 7 + u + 1), DEV),
                device_id_type=LOGICAL,
            )
        return carry

    lax.fori_loop(0, 18, greet, 0)
    pl.semaphore_signal(
        barrier,
        inc=1,
        device_id=lax.rem(me + DEV - 1, DEV),
        device_id_type=LOGICAL,
    )

    for copy in small[0:4]:
        copy.wait()
    owner = own_tile[...]
    owner_lat = lax.shift_right_logical(owner, 5)
    owner_lon = lax.bitwise_and(owner, 31)
    tiles = lax.broadcasted_iota(i32, (DEV, 256), 0)
    hit = jnp.where(tiles == owner, 1.0, 0.0)
    before = jnp.where(
        lax.broadcasted_iota(i32, (256, 256), 0)
        < lax.broadcasted_iota(i32, (256, 256), 1),
        1.0,
        0.0,
    )
    earlier = lax.dot_general(
        hit.astype(bf16), before.astype(bf16), NN, preferred_element_type=f32
    )
    rank = jnp.sum(hit * earlier, axis=0, keepdims=True).astype(i32)
    slot = owner_lat * 8 + rank
    slots = lax.broadcasted_iota(i32, (32, 256), 0)
    in_slot = slots == slot
    to_lon = jnp.where(slots == owner_lon, 1.0, 0.0).astype(bf16)
    zero = jnp.zeros((32, 256), f32)
    weights = 1.0 / own_error[...]
    spread = jnp.concatenate(
        [
            jnp.where(in_slot, value, zero)
            for value in (weights * own_value[...], weights, own_cell[...].astype(f32))
        ]
        + [zero],
        axis=0,
    )
    packed = jnp.zeros((LON, LANES), f32)
    for piece in thirds(spread):
        packed = packed + lax.dot_general(
            to_lon, piece, NT, preferred_element_type=f32
        )
    outbox[...] = packed

    for copy in small[4:6]:
        copy.wait()
    for group in range(GROUPS):
        for way in range(2):
            own_groups[way * GROUPS + group : way * GROUPS + group + 1, :] = own_courant[
                way : way + 1, group * GROUP : (group + 1) * GROUP
            ]
    number = lax.broadcasted_iota(i32, (16, LANES), 0) * LANES + lax.broadcasted_iota(
        i32, (16, LANES), 1
    )
    speed = jnp.concatenate(
        [own_courant[1:2, t * LANES : (t + 1) * LANES] for t in range(SPEC // LANES)]
        + [
            jnp.concatenate(
                [
                    own_courant[1:2, SPEC // LANES * LANES : SPEC],
                    jnp.zeros((1, LANES - SPEC % LANES), f32),
                ],
                axis=1,
            )
        ]
        + [jnp.zeros((15 - SPEC // LANES, LANES), f32)],
        axis=0,
    )
    backward = jnp.where(speed < 0.0, 1.0, 0.0).astype(bf16)
    upper = jnp.where(
        lax.broadcasted_iota(i32, (LANES, LANES), 0)
        <= lax.broadcasted_iota(i32, (LANES, LANES), 1),
        1.0,
        0.0,
    ).astype(bf16)
    within = lax.dot_general(backward, upper, NN, preferred_element_type=f32)
    whole = lax.dot_general(
        backward, jnp.ones((LANES, LANES), bf16), NN, preferred_element_type=f32
    )
    lower = jnp.where(
        lax.broadcasted_iota(i32, (16, 16), 1) < lax.broadcasted_iota(i32, (16, 16), 0),
        1.0,
        0.0,
    ).astype(bf16)
    south_upto = within + lax.dot_general(
        lower, whole.astype(bf16), NN, preferred_element_type=f32
    )
    beyond = number >= SPEC
    far = 4.0 * SPEC
    upto = (
        jnp.where(beyond, far, (number + 1).astype(f32) - south_upto),
        jnp.where(beyond, far, south_upto),
    )
    ones = jnp.ones((8, LANES), bf16)

    def enlist(turn, carry):
        place = (
            turn * LANES + lax.broadcasted_iota(i32, (LANES, LANES), 0)
        ).astype(f32)
        for side in range(2):
            count = jnp.zeros((LANES, LANES), f32)
            for t in range(SPEC // LANES + 1):
                count = count + jnp.where(upto[side][t : t + 1, :] <= place, 1.0, 0.0)
            total = lax.dot_general(
                ones, count.astype(bf16), NT, preferred_element_type=f32
            )
            listed[side, pl.ds(turn, 1), :] = jnp.maximum(
                jnp.minimum(total[0:1, :].astype(i32), SPEC - 1), 0
            )
        return carry

    lax.fori_loop(0, listed.shape[1], enlist, 0)
    to_scalars = pltpu.make_async_copy(listed, picks, list_sem)
    to_scalars.start()

    to_east = own_groups[0:GROUPS, :] < 0.0
    to_north = own_groups[GROUPS : 2 * GROUPS, :] < 0.0
    shape = (GROUPS, GROUP)
    group = lax.broadcasted_iota(i32, shape, 0)
    member = lax.broadcasted_iota(i32, shape, 1)
    number = group * GROUP + member
    backward = jnp.where(to_north, 1.0, 0.0).astype(bf16)
    upper = jnp.where(
        lax.broadcasted_iota(i32, (GROUP, GROUP), 0)
        < lax.broadcasted_iota(i32, (GROUP, GROUP), 1),
        1.0,
        0.0,
    ).astype(bf16)
    whole = lax.dot_general(
        backward, jnp.ones((GROUP, GROUP), bf16), NN, preferred_element_type=f32
    )
    lower = jnp.where(
        lax.broadcasted_iota(i32, (GROUPS, GROUPS), 1)
        < lax.broadcasted_iota(i32, (GROUPS, GROUPS), 0),
        1.0,
        0.0,
    ).astype(bf16)
    south = (
        lax.dot_general(backward, upper, NN, preferred_element_type=f32)
        + lax.dot_general(lower, whole.astype(bf16), NN, preferred_element_type=f32)
    ).astype(i32)
    plan[0] = jnp.where(to_east, LANES - 1, 1)
    plan[1] = jnp.where(
        to_east, LANES - 1 - member, jnp.where(member == 0, 0, LANES - member)
    )
    plan[2] = 8 + 16 * number + jnp.where(to_north, 1, -1)
    places[...] = 2 * jnp.where(to_north, cap + south, number - south)
    scalars = [
        pltpu.make_async_copy(plan, steps, small_sems.at[6]),
        pltpu.make_async_copy(own_groups, speeds, small_sems.at[7]),
    ]
    for copy in scalars:
        copy.start()
    cells[0:8, :] = jnp.zeros((8, LANES), f32)
    cells[8 + CELLS : 16 + CELLS, :] = jnp.zeros((8, LANES), f32)

    def pick_chunk(number):
        def pick(turn, carry):
            for u in range(8):
                at = number * CHUNK + turn * 8 + u
                line = lax.div(number, 2)
                spot = lax.rem(number, 2) * CHUNK + turn * 8 + u
                first = 8 + 16 * picks[0, line, spot]
                going_north[pl.ds(2 * at, 1), :] = cells[pl.ds(first + 7, 1), :]
                going_north[pl.ds(2 * at + 1, 1), :] = cells[pl.ds(first + 15, 1), :]
                first = 8 + 16 * picks[1, line, spot]
                going_south[pl.ds(2 * at, 1), :] = cells[pl.ds(first, 1), :]
                going_south[pl.ds(2 * at + 1, 1), :] = cells[pl.ds(first + 8, 1), :]
            return carry

        lax.fori_loop(0, CHUNK // 8, pick, 0)

    def north_copy(first, count):
        return pltpu.make_async_remote_copy(
            src_ref=going_north.at[pl.ds(first, count)],
            dst_ref=rows.at[pl.ds(first, count)],
            send_sem=row_sems.at[0],
            recv_sem=row_sems.at[1],
            device_id=(lat + 1, lon),
            device_id_type=MESH,
        )

    def south_copy(first, count):
        return pltpu.make_async_remote_copy(
            src_ref=going_south.at[pl.ds(first, count)],
            dst_ref=rows.at[pl.ds(2 * cap + first, count)],
            send_sem=row_sems.at[2],
            recv_sem=row_sems.at[3],
            device_id=(lat - 1, lon),
            device_id_type=MESH,
        )

    def send_chunk(number):
        first = pl.multiple_of(number * (2 * CHUNK), 2 * CHUNK)

        @pl.when(lat < LAT - 1)
        def _():
            north_copy(first, 2 * CHUNK).start()

        @pl.when(lat > 0)
        def _():
            south_copy(first, 2 * CHUNK).start()

    pl.semaphore_wait(barrier, DEV - 1)
    def post(turn, carry):
        for u in range(7):
            peer = lax.rem(me + (turn * 7 + u + 1), DEV)
            post_to(peer)
        return carry

    def post_to(peer):
        pltpu.make_async_remote_copy(
            src_ref=outbox.at[pl.ds(lax.rem(peer, LON), 1)],
            dst_ref=inbox.at[pl.ds(me, 1)],
            send_sem=box_sems.at[0],
            recv_sem=box_sems.at[1],
            device_id=peer,
            device_id_type=LOGICAL,
        ).start()

    lax.fori_loop(0, 18, post, 0)
    post_to(lax.rem(me + DEV - 1, DEV))
    inbox[pl.ds(me, 1), :] = outbox[pl.ds(lon, 1), :]

    for copy in loads:
        copy.wait()
    to_scalars.wait()
    for copy in scalars:
        copy.wait()
    pick_chunk(0)
    pick_chunk(1)
    send_chunk(0)
    send_chunk(1)

    lane = lax.broadcasted_iota(i32, (ROWS, LANES), 1)
    blank = jnp.zeros((ROWS, LANES), f32)

    def gather(pair, sums):
        sums = list(sums)
        for half in range(2):
            group = 2 * pair + half
            edge = blank
            for u in range(GROUP):
                at = 8 + (group * GROUP + u) * 16
                left = cells[pl.ds(pl.multiple_of(at, 8), ROWS), :]
                right = cells[pl.ds(pl.multiple_of(at + 8, 8), ROWS), :]
                k = 2 * (u % 4)
                sums[k] = sums[k] + left
                sums[k + 1] = sums[k + 1] + right
                speed = speeds[group, u]
                taken = jnp.where(jnp.full((ROWS, LANES), speed) < 0.0, left, right)
                turn = jnp.where(speed < 0.0, u, u + 1)
                edge = jnp.where(lane == u, pltpu.roll(taken, turn, 1), edge)
            own_edge[group] = edge
        return tuple(sums)

    sums = lax.fori_loop(0, GROUPS // 2, gather, tuple(blank for _ in range(8)))
    left = (sums[0] + sums[2]) + (sums[4] + sums[6])
    right = (sums[1] + sums[3]) + (sums[5] + sums[7])
    here_rows = pl.ds(pl.multiple_of(lat * ROWS, ROWS), ROWS)
    fields[2, here_rows, 0:LANES] = 4.0 * jnp.sqrt(left / SPEC)
    fields[2, here_rows, LANES:COLS] = 4.0 * jnp.sqrt(right / SPEC)
    fields[3, here_rows, 0:COLS] = own_sea[...].astype(f32)

    for step in range(1, LAT):
        peer = lax.rem(lat + step, LAT)
        part = fields.at[pl.ds(2, 2), here_rows, pl.ds(0, COLS)]
        pltpu.make_async_remote_copy(
            src_ref=part,
            dst_ref=part,
            send_sem=lat_sems.at[0],
            recv_sem=lat_sems.at[1],
            device_id=(peer, lon),
            device_id_type=MESH,
        ).start()

    send_west = pltpu.make_async_remote_copy(
        src_ref=own_edge,
        dst_ref=cols_east,
        send_sem=col_sems.at[0],
        recv_sem=col_sems.at[1],
        device_id=(lat, west),
        device_id_type=MESH,
    )
    send_east = pltpu.make_async_remote_copy(
        src_ref=own_edge,
        dst_ref=cols_west,
        send_sem=col_sems.at[2],
        recv_sem=col_sems.at[3],
        device_id=(lat, east),
        device_id_type=MESH,
    )
    send_west.start()
    send_east.start()

    pick_chunk(2)

    def forward(number, carry):
        pick_chunk(number)
        send_chunk(number - 1)
        return carry

    lax.fori_loop(3, chunks, forward, 0)

    @pl.when(lat == 0)
    def _():
        rows[0 : 2 * cap, :] = jnp.zeros((2 * cap, LANES), f32)

    @pl.when(lat == LAT - 1)
    def _():
        rows[2 * cap : 4 * cap, :] = jnp.zeros((2 * cap, LANES), f32)

    send_chunk(chunks - 1)

    got = pl.ds(0, DEV - 1)
    pltpu.make_async_copy(inbox.at[got], inbox.at[got], box_sems.at[1]).wait()
    turned[...] = inbox[...].T

    def place(number, carry):
        base = pl.multiple_of(number * 8, 8)
        misfits = turned[pl.ds(base, 8), :]
        weights = turned[pl.ds(base + 32, 8), :]
        cell = turned[pl.ds(base + 64, 8), :].astype(i32)
        cell_row = lax.shift_right_logical(cell, 8)
        cell_col = lax.bitwise_and(cell, 255)
        rows8 = lax.broadcasted_iota(i32, (8, LANES), 0)
        cols = lax.broadcasted_iota(i32, (COLS, LANES), 0)
        spots, sent = [], []
        for s in range(8):
            spots.append(jnp.where(cols == cell_col[s : s + 1, :], 1.0, 0.0).astype(bf16))
            at_row = rows8 == cell_row[s : s + 1, :]
            sent.append(
                jnp.concatenate(
                    [
                        jnp.where(at_row, misfits[s : s + 1, :], 0.0),
                        jnp.where(at_row, weights[s : s + 1, :], 0.0),
                    ],
                    axis=0,
                )
            )
        spots = jnp.concatenate(spots, axis=1)
        sent = jnp.concatenate(sent, axis=1)
        total = lax.dot_general(
            jnp.concatenate(thirds(sent), axis=0), spots, NT, preferred_element_type=f32
        )
        total = total[0:16, :] + total[16:32, :] + total[32:48, :]
        fields[0, pl.ds(base, 8), 0:COLS] = total[0:8, :]
        fields[1, pl.ds(base, 8), 0:COLS] = total[8:16, :]
        return carry

    lax.fori_loop(0, LAT, place, 0)

    three = fields.at[pl.ds(2, 2), pl.ds(0, NROW - ROWS), pl.ds(0, COLS)]
    pltpu.make_async_copy(three, three, lat_sems.at[1]).wait()
    pltpu.make_async_copy(three, three, lat_sems.at[0]).wait()
    height = fields[2, :, 0:COLS]
    ocean = fields[3, :, 0:COLS]
    weight = fields[1, :, 0:COLS] * ocean
    fields[0, :, 0:COLS] = (fields[0, :, 0:COLS] - height * fields[1, :, 0:COLS]) * ocean
    fields[1, :, 0:COLS] = weight

    rim_west = pltpu.make_async_remote_copy(
        src_ref=fields.at[pl.ds(0, 4), pl.ds(0, NROW), pl.ds(0, LANES)],
        dst_ref=near_east,
        send_sem=rim_sems.at[0],
        recv_sem=rim_sems.at[1],
        device_id=(lat, west),
        device_id_type=MESH,
    )
    rim_east = pltpu.make_async_remote_copy(
        src_ref=fields.at[pl.ds(0, 4), pl.ds(0, NROW), pl.ds(LANES, LANES)],
        dst_ref=near_west,
        send_sem=rim_sems.at[2],
        recv_sem=rim_sems.at[3],
        device_id=(lat, east),
        device_id_type=MESH,
    )
    rim_west.start()
    rim_east.start()
    rim_west.wait()
    rim_east.wait()
    lane = lax.broadcasted_iota(i32, (NROW, LANES), 1)
    for number, filler in enumerate((0.0, 0.0, 1.0, 0.0)):
        fields[number, :, COLS:EXT] = jnp.where(
            lane < RIM,
            near_east[number],
            jnp.where(lane >= LANES - RIM, near_west[number], filler),
        )

    row = lax.broadcasted_iota(i32, (NROW, EXT), 0)

    def north_of(x):
        return jnp.where(row == NROW - 1, 0.0, pltpu.roll(x, NROW - 1, 0))

    def south_of(x):
        return jnp.where(row == 0, 0.0, pltpu.roll(x, 1, 0))

    def east_of(x):
        return pltpu.roll(x, EXT - 1, 1)

    def west_of(x):
        return pltpu.roll(x, 1, 1)

    ocean = fields[3]
    share = spread_rate * ocean
    keep = 1.0 - share * (
        north_of(ocean) + south_of(ocean) + east_of(ocean) + west_of(ocean)
    )

    def relax(x):
        return keep * x + share * (
            (north_of(x) + south_of(x)) + (east_of(x) + west_of(x))
        )

    def relax_both(_, pair):
        return relax(pair[0]), relax(pair[1])

    misfit, weight = lax.fori_loop(0, PASSES, relax_both, (fields[0], fields[1]))
    increment = ocean * misfit / (prior_weight + weight)
    factor = jnp.exp(2.0 * increment / fields[2]) * ocean
    going_up = factor * north_of(ocean)
    going_down = factor * south_of(ocean)
    for number, value in enumerate(
        (
            factor,
            factor * east_of(ocean),
            factor * west_of(ocean),
            going_up,
            going_down,
            south_of(going_up),
            north_of(going_down),
            increment,
        )
    ):
        padded[number] = value
    own = here_rows
    sub = lax.broadcasted_iota(i32, (ROWS, LANES), 0)
    for number in range(7):
        for half in range(2):
            value = padded[number, own, half * LANES : (half + 1) * LANES]
            if number == 5:
                rim_tables[8 * half : 8 * half + 8, :] = jnp.where(sub == 0, value, 0.0)
                value = jnp.where(sub == 0, 0.0, value)
            if number == 6:
                outer = sub == ROWS - 1
                rim_tables[16 + 8 * half : 24 + 8 * half, :] = jnp.where(
                    outer, value, 0.0
                )
                value = jnp.where(outer, 0.0, value)
            tables[16 * number + 8 * half : 16 * number + 8 * half + 8, :] = value
    increments[...] = padded[7, own, 0:COLS]
    beside = (
        jnp.broadcast_to(padded[1, own, EXT - 1 : EXT], (ROWS, LANES)),
        jnp.broadcast_to(padded[2, own, COLS : COLS + 1], (ROWS, LANES)),
    )

    send_west.wait()
    send_east.wait()

    def advance(step, carry):
        rims = cols_west[step] * beside[0], cols_east[step] * beside[1]
        for u in range(GROUP):
            at = 8 + (step * GROUP + u) * 16
            near = steps[2, step, u]
            speed = jnp.full((ROWS, LANES), speeds[step, u])
            back = speed < 0.0
            cell, flow = [], []
            for half in range(2):
                first = 8 * half
                cell.append(cells[pl.ds(pl.multiple_of(at + first, 8), 8), :])
                way = jnp.where(
                    back, tables[32 + first : 40 + first, :], tables[16 + first : 24 + first, :]
                )
                flow.append(cell[half] * way)
            shift = steps[0, step, u]
            moved = pltpu.roll(flow[0], shift, 1), pltpu.roll(flow[1], shift, 1)
            rim = pltpu.roll(jnp.where(back, rims[1], rims[0]), steps[1, step, u], 1)
            at_edge = lane == jnp.where(back, LANES - 1, 0)
            came = (
                jnp.where(at_edge, jnp.where(back, moved[1], rim), moved[0]),
                jnp.where(at_edge, jnp.where(back, rim, moved[0]), moved[1]),
            )
            speed = jnp.abs(speed)
            slow = jnp.full((ROWS, LANES), speeds[GROUPS + step, u])
            down = slow < 0.0
            slow = jnp.abs(slow)
            for half in range(2):
                first = 8 * half
                way = jnp.where(
                    down, tables[64 + first : 72 + first, :], tables[48 + first : 56 + first, :]
                )
                way_in = jnp.where(
                    down, tables[96 + first : 104 + first, :], tables[80 + first : 88 + first, :]
                )
                gone = cell[half] * way - cells[pl.ds(near + first, 8), :] * way_in
                to = pl.multiple_of((step * GROUP + u) * 16 + first, 8)
                partial[pl.ds(to, 8), :] = (
                    cell[half] * tables[first : first + 8, :]
                    - speed * (flow[half] - came[half])
                    - slow * gone
                )
        return carry

    lane = lax.broadcasted_iota(i32, (ROWS, LANES), 1)
    lax.fori_loop(0, GROUPS, advance, 0)

    pltpu.make_async_copy(inbox.at[got], inbox.at[got], box_sems.at[0]).wait()

    @pl.when(lat < LAT - 1)
    def _():
        north_copy(0, 2 * cap).wait_send()
        part = rows.at[pl.ds(2 * cap, 2 * cap)]
        pltpu.make_async_copy(part, part, row_sems.at[3]).wait()

    @pl.when(lat > 0)
    def _():
        south_copy(0, 2 * cap).wait_send()
        part = rows.at[pl.ds(0, 2 * cap)]
        pltpu.make_async_copy(part, part, row_sems.at[1]).wait()


def exchange(cap, spectrum, courant, *observed):
    vmem = pl.BlockSpec(memory_space=pltpu.VMEM)
    lists = -(-cap // LANES)
    return pl.pallas_call(
        functools.partial(exchange_kernel, cap),
        out_shape=(
            jax.ShapeDtypeStruct((CELLS, LANES), f32),
            jax.ShapeDtypeStruct((32, LANES), f32),
            jax.ShapeDtypeStruct((ROWS, COLS), f32),
            jax.ShapeDtypeStruct((4 * cap, LANES), f32),
            jax.ShapeDtypeStruct((GROUPS, GROUP), i32),
            jax.ShapeDtypeStruct((2 * GROUPS, GROUP), f32),
        ),
        in_specs=[pl.BlockSpec(memory_space=pl.ANY)] * 7,
        out_specs=(vmem,) * 6,
        scratch_shapes=[
            pltpu.VMEM((CELLS + 16, LANES), f32),
            pltpu.VMEM((112, LANES), f32),
            pltpu.VMEM((GROUPS, ROWS, LANES), f32),
            pltpu.VMEM((GROUPS, ROWS, LANES), f32),
            pltpu.VMEM((3, GROUPS, GROUP), i32),
            pltpu.SMEM((3, GROUPS, GROUP), i32),
            pltpu.SMEM((2 * GROUPS, GROUP), f32),
            pltpu.VMEM((2, SPEC), f32),
            pltpu.VMEM((1, 256), i32),
            pltpu.VMEM((1, 256), i32),
            pltpu.VMEM((1, 256), f32),
            pltpu.VMEM((1, 256), f32),
            pltpu.VMEM((ROWS, COLS), i32),
            pltpu.VMEM((LON, LANES), f32),
            pltpu.VMEM((DEV, LANES), f32),
            pltpu.VMEM((LANES, DEV), f32),
            pltpu.VMEM((4, NROW, EXT), f32),
            pltpu.VMEM((4, NROW, LANES), f32),
            pltpu.VMEM((4, NROW, LANES), f32),
            pltpu.VMEM((GROUPS, ROWS, LANES), f32),
            pltpu.VMEM((8, NROW, EXT), f32),
            pltpu.VMEM((2 * cap, LANES), f32),
            pltpu.VMEM((2 * cap, LANES), f32),
            pltpu.VMEM((2, lists, LANES), i32),
            pltpu.SMEM((2, lists, LANES), i32),
            pltpu.SemaphoreType.DMA((LOADS,)),
            pltpu.SemaphoreType.DMA((8,)),
            pltpu.SemaphoreType.DMA,
            pltpu.SemaphoreType.DMA((2,)),
            pltpu.SemaphoreType.DMA((2,)),
            pltpu.SemaphoreType.DMA((4,)),
            pltpu.SemaphoreType.DMA((4,)),
            pltpu.SemaphoreType.DMA((4,)),
        ],
        compiler_params=pltpu.CompilerParams(
            collective_id=0 if cap == CAP_HALF else 1,
            has_side_effects=True,
            vmem_limit_bytes=30 * 2**20,
        ),
        name=f"exchange_{cap}",
    )(spectrum, courant, *observed)


def update_kernel(
    partial, rim_tables, increments, rows, places, speeds, out, increment, place, speed, sems
):
    step = pl.program_id(0)

    @pl.when(step == 0)
    def _():
        copies = [
            pltpu.make_async_copy(places, place, sems.at[0]),
            pltpu.make_async_copy(speeds, speed, sems.at[1]),
        ]
        for copy in copies:
            copy.start()
        increment[...] = increments[...]
        for copy in copies:
            copy.wait()

    for u in range(GROUP):
        at = (step * GROUP + u) * 16
        slow = jnp.full((ROWS, LANES), speed[GROUPS + step, u])
        down = slow < 0.0
        slow = jnp.abs(slow)
        line = place[step, u]
        for half in range(2):
            first = 8 * half
            way = jnp.where(
                down, rim_tables[16 + first : 24 + first, :], rim_tables[first : first + 8, :]
            )
            row = jnp.broadcast_to(rows[pl.ds(line + half, 1), :], (ROWS, LANES))
            out[u * 16 + first : u * 16 + first + 8, :] = (
                partial[pl.ds(pl.multiple_of(at + first, 8), 8), :] + slow * (row * way)
            )


def update(cap, *sent):
    vmem = pl.BlockSpec(memory_space=pltpu.VMEM)
    return pl.pallas_call(
        update_kernel,
        grid=(GROUPS,),
        out_shape=(
            jax.ShapeDtypeStruct((CELLS, LANES), f32),
            jax.ShapeDtypeStruct((ROWS, COLS), f32),
        ),
        in_specs=[vmem] * 6,
        out_specs=(
            pl.BlockSpec((GROUP * 16, LANES), lambda i: (i, 0)),
            pl.BlockSpec((ROWS, COLS), lambda i: (0, 0)),
        ),
        scratch_shapes=[
            pltpu.SMEM((GROUPS, GROUP), i32),
            pltpu.SMEM((2 * GROUPS, GROUP), f32),
            pltpu.SemaphoreType.DMA((2,)),
        ],
        compiler_params=pltpu.CompilerParams(
            dimension_semantics=("arbitrary",), vmem_limit_bytes=24 * 2**20
        ),
        name=f"update_{cap}",
    )(*sent)


def body(spectrum, sea_mask, courant, obs_tile, obs_cell, obs_value, obs_error):
    halves = spectrum.reshape(SPEC, ROWS, 2, LANES).transpose(0, 2, 1, 3)
    observed = (
        obs_tile.reshape(1, -1),
        obs_cell.reshape(1, -1),
        obs_value.reshape(1, -1),
        obs_error.reshape(1, -1),
        sea_mask,
    )
    south = jnp.sum((courant[1] < 0.0).astype(i32))
    fits = jnp.maximum(south, SPEC - south) <= CAP_HALF

    def run(cap):
        sent = exchange(cap, halves.reshape(CELLS, LANES), courant, *observed)
        return update(cap, *sent)

    updated, increment = lax.cond(fits, lambda: run(CAP_HALF), lambda: run(CAP_ALL))
    updated = updated.reshape(SPEC, 2, ROWS, LANES).transpose(0, 2, 1, 3)
    return updated.reshape(SPEC, ROWS, COLS), increment


def solution(mesh):
    return jax.shard_map(
        body,
        mesh=mesh,
        in_specs=(
            P(None, "lat", "lon"),
            P("lat", "lon"),
            P(),
            P(("lat", "lon"), None),
            P(("lat", "lon")),
            P(("lat", "lon")),
            P(("lat", "lon")),
        ),
        out_specs=(P(None, "lat", "lon"), P("lat", "lon")),
        check_vma=False,
    )
```

```python
import functools

import jax
import jax.numpy as jnp
from jax import lax
from jax.experimental import pallas as pl
from jax.experimental.pallas import tpu as pltpu
from jax.sharding import PartitionSpec as P

SPEC = 1296
ROWS = 8
COLS = 256
LAT = 4
LON = 32
DEV = LAT * LON
NROW = LAT * ROWS
PASSES = 8
LANES = 128
GROUP = 72
GROUPS = SPEC // GROUP
CELLS = SPEC * 16
LOADS = 6
EXT = 384
RIM = 9
CHUNK = 64
CAP_HALF = 704
CAP_ALL = 1344

spread_rate = 0.2
prior_weight = 4.0

f32 = jnp.float32
i32 = jnp.int32
bf16 = jnp.bfloat16
MESH = pl.DeviceIdType.MESH
LOGICAL = pl.DeviceIdType.LOGICAL
NT = (((1,), (1,)), ((), ()))
NN = (((1,), (0,)), ((), ()))


def thirds(x):
    high = x.astype(bf16)
    rest = x - high.astype(f32)
    mid = rest.astype(bf16)
    low = (rest - mid.astype(f32)).astype(bf16)
    return high, mid, low


def exchange_kernel(
    cap,
    spectrum,
    courant,
    obs_tile,
    obs_cell,
    obs_value,
    obs_error,
    sea,
    partial,
    rim_tables,
    increments,
    rows,
    places,
    own_groups,
    cells,
    tables,
    cols_west,
    cols_east,
    plan,
    steps,
    speeds,
    own_courant,
    own_tile,
    own_cell,
    own_value,
    own_error,
    own_sea,
    outbox,
    inbox,
    turned,
    fields,
    near_west,
    near_east,
    own_edge,
    padded,
    going_north,
    going_south,
    listed,
    picks,
    load_sems,
    small_sems,
    list_sem,
    box_sems,
    lat_sems,
    col_sems,
    rim_sems,
    row_sems,
):
    lat = lax.axis_index("lat")
    lon = lax.axis_index("lon")
    me = lat * LON + lon
    west = lax.rem(lon + LON - 1, LON)
    east = lax.rem(lon + 1, LON)
    chunks = cap // CHUNK

    small = [
        pltpu.make_async_copy(source, target, small_sems.at[number])
        for number, (source, target) in enumerate(
            (
                (obs_tile, own_tile),
                (obs_error, own_error),
                (obs_value, own_value),
                (obs_cell, own_cell),
                (courant, own_courant),
                (sea, own_sea),
            )
        )
    ]
    for copy in small:
        copy.start()
    size = CELLS // LOADS
    loads = [
        pltpu.make_async_copy(
            spectrum.at[pl.ds(part * size, size)],
            cells.at[pl.ds(8 + part * size, size)],
            load_sems.at[part],
        )
        for part in range(LOADS)
    ]
    for copy in loads:
        copy.start()

    barrier = pltpu.get_barrier_semaphore()

    def greet(turn, carry):
        for u in range(7):
            pl.semaphore_signal(
                barrier,
                inc=1,
                device_id=lax.rem(me + (turn * 7 + u + 1), DEV),
                device_id_type=LOGICAL,
            )
        return carry

    lax.fori_loop(0, 18, greet, 0)
    pl.semaphore_signal(
        barrier,
        inc=1,
        device_id=lax.rem(me + DEV - 1, DEV),
        device_id_type=LOGICAL,
    )

    for copy in small[4:6]:
        copy.wait()
    number = lax.broadcasted_iota(i32, (16, LANES), 0) * LANES + lax.broadcasted_iota(
        i32, (16, LANES), 1
    )
    speed = jnp.concatenate(
        [own_courant[1:2, t * LANES : (t + 1) * LANES] for t in range(SPEC // LANES)]
        + [
            jnp.concatenate(
                [
                    own_courant[1:2, SPEC // LANES * LANES : SPEC],
                    jnp.zeros((1, LANES - SPEC % LANES), f32),
                ],
                axis=1,
            )
        ]
        + [jnp.zeros((15 - SPEC // LANES, LANES), f32)],
        axis=0,
    )
    backward = jnp.where(speed < 0.0, 1.0, 0.0).astype(bf16)
    upper = jnp.where(
        lax.broadcasted_iota(i32, (LANES, LANES), 0)
        <= lax.broadcasted_iota(i32, (LANES, LANES), 1),
        1.0,
        0.0,
    ).astype(bf16)
    within = lax.dot_general(backward, upper, NN, preferred_element_type=f32)
    whole = lax.dot_general(
        backward, jnp.ones((LANES, LANES), bf16), NN, preferred_element_type=f32
    )
    lower = jnp.where(
        lax.broadcasted_iota(i32, (16, 16), 1) < lax.broadcasted_iota(i32, (16, 16), 0),
        1.0,
        0.0,
    ).astype(bf16)
    south_upto = within + lax.dot_general(
        lower, whole.astype(bf16), NN, preferred_element_type=f32
    )
    beyond = number >= SPEC
    far = 4.0 * SPEC
    upto = (
        jnp.where(beyond, far, (number + 1).astype(f32) - south_upto),
        jnp.where(beyond, far, south_upto),
    )
    ones = jnp.ones((8, LANES), bf16)

    def enlist(turn, carry):
        place = (
            turn * LANES + lax.broadcasted_iota(i32, (LANES, LANES), 0)
        ).astype(f32)
        for side in range(2):
            count = jnp.zeros((LANES, LANES), f32)
            for t in range(SPEC // LANES + 1):
                count = count + jnp.where(upto[side][t : t + 1, :] <= place, 1.0, 0.0)
            total = lax.dot_general(
                ones, count.astype(bf16), NT, preferred_element_type=f32
            )
            listed[side, pl.ds(turn, 1), :] = jnp.maximum(
                jnp.minimum(total[0:1, :].astype(i32), SPEC - 1), 0
            )
        return carry

    lax.fori_loop(0, listed.shape[1], enlist, 0)
    to_scalars = pltpu.make_async_copy(listed, picks, list_sem)
    to_scalars.start()

    def pick_chunk(number):
        def pick(turn, carry):
            for u in range(8):
                at = number * CHUNK + turn * 8 + u
                line = lax.div(number, 2)
                spot = lax.rem(number, 2) * CHUNK + turn * 8 + u
                first = 8 + 16 * picks[0, line, spot]
                going_north[pl.ds(2 * at, 1), :] = cells[pl.ds(first + 7, 1), :]
                going_north[pl.ds(2 * at + 1, 1), :] = cells[pl.ds(first + 15, 1), :]
                first = 8 + 16 * picks[1, line, spot]
                going_south[pl.ds(2 * at, 1), :] = cells[pl.ds(first, 1), :]
                going_south[pl.ds(2 * at + 1, 1), :] = cells[pl.ds(first + 8, 1), :]
            return carry

        lax.fori_loop(0, CHUNK // 8, pick, 0)

    def north_copy(first, count):
        return pltpu.make_async_remote_copy(
            src_ref=going_north.at[pl.ds(first, count)],
            dst_ref=rows.at[pl.ds(first, count)],
            send_sem=row_sems.at[0],
            recv_sem=row_sems.at[1],
            device_id=(lat + 1, lon),
            device_id_type=MESH,
        )

    def south_copy(first, count):
        return pltpu.make_async_remote_copy(
            src_ref=going_south.at[pl.ds(first, count)],
            dst_ref=rows.at[pl.ds(2 * cap + first, count)],
            send_sem=row_sems.at[2],
            recv_sem=row_sems.at[3],
            device_id=(lat - 1, lon),
            device_id_type=MESH,
        )

    def send_chunk(number):
        first = pl.multiple_of(number * (2 * CHUNK), 2 * CHUNK)

        @pl.when(lat < LAT - 1)
        def _():
            north_copy(first, 2 * CHUNK).start()

        @pl.when(lat > 0)
        def _():
            south_copy(first, 2 * CHUNK).start()

    for copy in loads:
        copy.wait()
    to_scalars.wait()
    pick_chunk(0)
    pick_chunk(1)
    pick_chunk(2)
    pl.semaphore_wait(barrier, DEV - 1)
    for number in range(3):
        send_chunk(number)

    for copy in small[0:4]:
        copy.wait()
    owner = own_tile[...]
    owner_lat = lax.shift_right_logical(owner, 5)
    owner_lon = lax.bitwise_and(owner, 31)
    tiles = lax.broadcasted_iota(i32, (DEV, 256), 0)
    hit = jnp.where(tiles == owner, 1.0, 0.0)
    before = jnp.where(
        lax.broadcasted_iota(i32, (256, 256), 0)
        < lax.broadcasted_iota(i32, (256, 256), 1),
        1.0,
        0.0,
    )
    earlier = lax.dot_general(
        hit.astype(bf16), before.astype(bf16), NN, preferred_element_type=f32
    )
    rank = jnp.sum(hit * earlier, axis=0, keepdims=True).astype(i32)
    slot = owner_lat * 8 + rank
    slots = lax.broadcasted_iota(i32, (32, 256), 0)
    in_slot = slots == slot
    to_lon = jnp.where(slots == owner_lon, 1.0, 0.0).astype(bf16)
    zero = jnp.zeros((32, 256), f32)
    weights = 1.0 / own_error[...]
    spread = jnp.concatenate(
        [
            jnp.where(in_slot, value, zero)
            for value in (weights * own_value[...], weights, own_cell[...].astype(f32))
        ]
        + [zero],
        axis=0,
    )
    packed = jnp.zeros((LON, LANES), f32)
    for piece in thirds(spread):
        packed = packed + lax.dot_general(
            to_lon, piece, NT, preferred_element_type=f32
        )
    outbox[...] = packed

    def post(turn, carry):
        for u in range(7):
            peer = lax.rem(me + (turn * 7 + u + 1), DEV)
            post_to(peer)
        return carry

    def post_to(peer):
        pltpu.make_async_remote_copy(
            src_ref=outbox.at[pl.ds(lax.rem(peer, LON), 1)],
            dst_ref=inbox.at[pl.ds(me, 1)],
            send_sem=box_sems.at[0],
            recv_sem=box_sems.at[1],
            device_id=peer,
            device_id_type=LOGICAL,
        ).start()

    lax.fori_loop(0, 18, post, 0)
    post_to(lax.rem(me + DEV - 1, DEV))
    inbox[pl.ds(me, 1), :] = outbox[pl.ds(lon, 1), :]

    for group in range(GROUPS):
        for way in range(2):
            own_groups[way * GROUPS + group : way * GROUPS + group + 1, :] = own_courant[
                way : way + 1, group * GROUP : (group + 1) * GROUP
            ]
    to_east = own_groups[0:GROUPS, :] < 0.0
    to_north = own_groups[GROUPS : 2 * GROUPS, :] < 0.0
    shape = (GROUPS, GROUP)
    group = lax.broadcasted_iota(i32, shape, 0)
    member = lax.broadcasted_iota(i32, shape, 1)
    number = group * GROUP + member
    backward = jnp.where(to_north, 1.0, 0.0).astype(bf16)
    upper = jnp.where(
        lax.broadcasted_iota(i32, (GROUP, GROUP), 0)
        < lax.broadcasted_iota(i32, (GROUP, GROUP), 1),
        1.0,
        0.0,
    ).astype(bf16)
    whole = lax.dot_general(
        backward, jnp.ones((GROUP, GROUP), bf16), NN, preferred_element_type=f32
    )
    lower = jnp.where(
        lax.broadcasted_iota(i32, (GROUPS, GROUPS), 1)
        < lax.broadcasted_iota(i32, (GROUPS, GROUPS), 0),
        1.0,
        0.0,
    ).astype(bf16)
    south = (
        lax.dot_general(backward, upper, NN, preferred_element_type=f32)
        + lax.dot_general(lower, whole.astype(bf16), NN, preferred_element_type=f32)
    ).astype(i32)
    plan[0] = jnp.where(to_east, LANES - 1, 1)
    plan[1] = jnp.where(
        to_east, LANES - 1 - member, jnp.where(member == 0, 0, LANES - member)
    )
    plan[2] = 8 + 16 * number + jnp.where(to_north, 1, -1)
    places[...] = 2 * jnp.where(to_north, cap + south, number - south)
    scalars = [
        pltpu.make_async_copy(plan, steps, small_sems.at[6]),
        pltpu.make_async_copy(own_groups, speeds, small_sems.at[7]),
    ]
    for copy in scalars:
        copy.start()
    cells[0:8, :] = jnp.zeros((8, LANES), f32)
    cells[8 + CELLS : 16 + CELLS, :] = jnp.zeros((8, LANES), f32)

    for copy in scalars:
        copy.wait()

    lane = lax.broadcasted_iota(i32, (ROWS, LANES), 1)
    blank = jnp.zeros((ROWS, LANES), f32)

    def gather(pair, sums):
        sums = list(sums)
        for half in range(2):
            group = 2 * pair + half
            edge = blank
            for u in range(GROUP):
                at = 8 + (group * GROUP + u) * 16
                left = cells[pl.ds(pl.multiple_of(at, 8), ROWS), :]
                right = cells[pl.ds(pl.multiple_of(at + 8, 8), ROWS), :]
                k = 2 * (u % 4)
                sums[k] = sums[k] + left
                sums[k + 1] = sums[k + 1] + right
                speed = speeds[group, u]
                taken = jnp.where(jnp.full((ROWS, LANES), speed) < 0.0, left, right)
                turn = jnp.where(speed < 0.0, u, u + 1)
                edge = jnp.where(lane == u, pltpu.roll(taken, turn, 1), edge)
            own_edge[group] = edge
        return tuple(sums)

    sums = lax.fori_loop(0, GROUPS // 2, gather, tuple(blank for _ in range(8)))
    left = (sums[0] + sums[2]) + (sums[4] + sums[6])
    right = (sums[1] + sums[3]) + (sums[5] + sums[7])
    here_rows = pl.ds(pl.multiple_of(lat * ROWS, ROWS), ROWS)
    fields[2, here_rows, 0:LANES] = 4.0 * jnp.sqrt(left / SPEC)
    fields[2, here_rows, LANES:COLS] = 4.0 * jnp.sqrt(right / SPEC)
    fields[3, here_rows, 0:COLS] = own_sea[...].astype(f32)

    for step in range(1, LAT):
        peer = lax.rem(lat + step, LAT)
        part = fields.at[pl.ds(2, 2), here_rows, pl.ds(0, COLS)]
        pltpu.make_async_remote_copy(
            src_ref=part,
            dst_ref=part,
            send_sem=lat_sems.at[0],
            recv_sem=lat_sems.at[1],
            device_id=(peer, lon),
            device_id_type=MESH,
        ).start()

    send_west = pltpu.make_async_remote_copy(
        src_ref=own_edge,
        dst_ref=cols_east,
        send_sem=col_sems.at[0],
        recv_sem=col_sems.at[1],
        device_id=(lat, west),
        device_id_type=MESH,
    )
    send_east = pltpu.make_async_remote_copy(
        src_ref=own_edge,
        dst_ref=cols_west,
        send_sem=col_sems.at[2],
        recv_sem=col_sems.at[3],
        device_id=(lat, east),
        device_id_type=MESH,
    )
    send_west.start()
    send_east.start()

    pick_chunk(3)

    def forward(number, carry):
        pick_chunk(number)
        send_chunk(number - 1)
        return carry

    early = chunks * 7 // 11
    lax.fori_loop(4, early, forward, 0)

    @pl.when(lat == 0)
    def _():
        rows[0 : 2 * cap, :] = jnp.zeros((2 * cap, LANES), f32)

    @pl.when(lat == LAT - 1)
    def _():
        rows[2 * cap : 4 * cap, :] = jnp.zeros((2 * cap, LANES), f32)

    def rim_copies(first, sems):
        part = pl.ds(first, 2)
        return (
            pltpu.make_async_remote_copy(
                src_ref=fields.at[part, pl.ds(0, NROW), pl.ds(0, LANES)],
                dst_ref=near_east.at[part],
                send_sem=rim_sems.at[sems],
                recv_sem=rim_sems.at[sems + 1],
                device_id=(lat, west),
                device_id_type=MESH,
            ),
            pltpu.make_async_remote_copy(
                src_ref=fields.at[part, pl.ds(0, NROW), pl.ds(LANES, LANES)],
                dst_ref=near_west.at[part],
                send_sem=rim_sems.at[sems + 2],
                recv_sem=rim_sems.at[sems + 3],
                device_id=(lat, east),
                device_id_type=MESH,
            ),
        )

    got = pl.ds(0, DEV - 1)
    pltpu.make_async_copy(inbox.at[got], inbox.at[got], box_sems.at[1]).wait()
    turned[...] = inbox[...].T

    def place(number, carry):
        base = pl.multiple_of(number * 8, 8)
        misfits = turned[pl.ds(base, 8), :]
        weights = turned[pl.ds(base + 32, 8), :]
        cell = turned[pl.ds(base + 64, 8), :].astype(i32)
        cell_row = lax.shift_right_logical(cell, 8)
        cell_col = lax.bitwise_and(cell, 255)
        rows8 = lax.broadcasted_iota(i32, (8, LANES), 0)
        cols = lax.broadcasted_iota(i32, (COLS, LANES), 0)
        spots, sent = [], []
        for s in range(8):
            spots.append(jnp.where(cols == cell_col[s : s + 1, :], 1.0, 0.0).astype(bf16))
            at_row = rows8 == cell_row[s : s + 1, :]
            sent.append(
                jnp.concatenate(
                    [
                        jnp.where(at_row, misfits[s : s + 1, :], 0.0),
                        jnp.where(at_row, weights[s : s + 1, :], 0.0),
                    ],
                    axis=0,
                )
            )
        spots = jnp.concatenate(spots, axis=1)
        sent = jnp.concatenate(sent, axis=1)
        total = lax.dot_general(
            jnp.concatenate(thirds(sent), axis=0), spots, NT, preferred_element_type=f32
        )
        total = total[0:16, :] + total[16:32, :] + total[32:48, :]
        fields[0, pl.ds(base, 8), 0:COLS] = total[0:8, :]
        fields[1, pl.ds(base, 8), 0:COLS] = total[8:16, :]
        return carry

    lax.fori_loop(0, LAT, place, 0)

    three = fields.at[pl.ds(2, 2), pl.ds(0, NROW - ROWS), pl.ds(0, COLS)]
    pltpu.make_async_copy(three, three, lat_sems.at[1]).wait()
    pltpu.make_async_copy(three, three, lat_sems.at[0]).wait()
    coast_rims = rim_copies(2, 0)
    for copy in coast_rims:
        copy.start()
    height = fields[2, :, 0:COLS]
    ocean = fields[3, :, 0:COLS]
    weight = fields[1, :, 0:COLS] * ocean
    fields[0, :, 0:COLS] = (fields[0, :, 0:COLS] - height * fields[1, :, 0:COLS]) * ocean
    fields[1, :, 0:COLS] = weight
    field_rims = rim_copies(0, 4)
    for copy in field_rims:
        copy.start()
    lax.fori_loop(early, chunks, forward, 0)
    send_chunk(chunks - 1)
    for copy in coast_rims + field_rims:
        copy.wait()
    lane = lax.broadcasted_iota(i32, (NROW, LANES), 1)
    for number, filler in enumerate((0.0, 0.0, 1.0, 0.0)):
        fields[number, :, COLS:EXT] = jnp.where(
            lane < RIM,
            near_east[number],
            jnp.where(lane >= LANES - RIM, near_west[number], filler),
        )

    row = lax.broadcasted_iota(i32, (NROW, EXT), 0)

    def north_of(x):
        return jnp.where(row == NROW - 1, 0.0, pltpu.roll(x, NROW - 1, 0))

    def south_of(x):
        return jnp.where(row == 0, 0.0, pltpu.roll(x, 1, 0))

    def east_of(x):
        return pltpu.roll(x, EXT - 1, 1)

    def west_of(x):
        return pltpu.roll(x, 1, 1)

    ocean = fields[3]
    share = spread_rate * ocean
    keep = 1.0 - share * (
        north_of(ocean) + south_of(ocean) + east_of(ocean) + west_of(ocean)
    )

    def relax(x):
        return keep * x + share * (
            (north_of(x) + south_of(x)) + (east_of(x) + west_of(x))
        )

    def relax_both(_, pair):
        return relax(pair[0]), relax(pair[1])

    misfit, weight = lax.fori_loop(0, PASSES, relax_both, (fields[0], fields[1]))
    increment = ocean * misfit / (prior_weight + weight)
    factor = jnp.exp(2.0 * increment / fields[2]) * ocean
    going_up = factor * north_of(ocean)
    going_down = factor * south_of(ocean)
    for number, value in enumerate(
        (
            factor,
            factor * east_of(ocean),
            factor * west_of(ocean),
            going_up,
            going_down,
            south_of(going_up),
            north_of(going_down),
            increment,
        )
    ):
        padded[number] = value
    own = here_rows
    sub = lax.broadcasted_iota(i32, (ROWS, LANES), 0)
    for number in range(7):
        for half in range(2):
            value = padded[number, own, half * LANES : (half + 1) * LANES]
            if number == 5:
                rim_tables[8 * half : 8 * half + 8, :] = jnp.where(sub == 0, value, 0.0)
                value = jnp.where(sub == 0, 0.0, value)
            if number == 6:
                outer = sub == ROWS - 1
                rim_tables[16 + 8 * half : 24 + 8 * half, :] = jnp.where(
                    outer, value, 0.0
                )
                value = jnp.where(outer, 0.0, value)
            tables[16 * number + 8 * half : 16 * number + 8 * half + 8, :] = value
    increments[...] = padded[7, own, 0:COLS]
    beside = (
        jnp.broadcast_to(padded[1, own, EXT - 1 : EXT], (ROWS, LANES)),
        jnp.broadcast_to(padded[2, own, COLS : COLS + 1], (ROWS, LANES)),
    )

    send_west.wait()
    send_east.wait()

    def advance(step, carry):
        rims = cols_west[step] * beside[0], cols_east[step] * beside[1]
        for u in range(GROUP):
            at = 8 + (step * GROUP + u) * 16
            near = steps[2, step, u]
            speed = jnp.full((ROWS, LANES), speeds[step, u])
            back = speed < 0.0
            cell, flow = [], []
            for half in range(2):
                first = 8 * half
                cell.append(cells[pl.ds(pl.multiple_of(at + first, 8), 8), :])
                way = jnp.where(
                    back, tables[32 + first : 40 + first, :], tables[16 + first : 24 + first, :]
                )
                flow.append(cell[half] * way)
            shift = steps[0, step, u]
            moved = pltpu.roll(flow[0], shift, 1), pltpu.roll(flow[1], shift, 1)
            rim = pltpu.roll(jnp.where(back, rims[1], rims[0]), steps[1, step, u], 1)
            at_edge = lane == jnp.where(back, LANES - 1, 0)
            came = (
                jnp.where(at_edge, jnp.where(back, moved[1], rim), moved[0]),
                jnp.where(at_edge, jnp.where(back, rim, moved[0]), moved[1]),
            )
            speed = jnp.abs(speed)
            slow = jnp.full((ROWS, LANES), speeds[GROUPS + step, u])
            down = slow < 0.0
            slow = jnp.abs(slow)
            for half in range(2):
                first = 8 * half
                way = jnp.where(
                    down, tables[64 + first : 72 + first, :], tables[48 + first : 56 + first, :]
                )
                way_in = jnp.where(
                    down, tables[96 + first : 104 + first, :], tables[80 + first : 88 + first, :]
                )
                gone = cell[half] * way - cells[pl.ds(near + first, 8), :] * way_in
                to = pl.multiple_of((step * GROUP + u) * 16 + first, 8)
                partial[pl.ds(to, 8), :] = (
                    cell[half] * tables[first : first + 8, :]
                    - speed * (flow[half] - came[half])
                    - slow * gone
                )
        return carry

    lane = lax.broadcasted_iota(i32, (ROWS, LANES), 1)
    lax.fori_loop(0, GROUPS, advance, 0)

    pltpu.make_async_copy(inbox.at[got], inbox.at[got], box_sems.at[0]).wait()

    @pl.when(lat < LAT - 1)
    def _():
        north_copy(0, 2 * cap).wait_send()
        part = rows.at[pl.ds(2 * cap, 2 * cap)]
        pltpu.make_async_copy(part, part, row_sems.at[3]).wait()

    @pl.when(lat > 0)
    def _():
        south_copy(0, 2 * cap).wait_send()
        part = rows.at[pl.ds(0, 2 * cap)]
        pltpu.make_async_copy(part, part, row_sems.at[1]).wait()


def exchange(cap, spectrum, courant, *observed):
    vmem = pl.BlockSpec(memory_space=pltpu.VMEM)
    lists = -(-cap // LANES)
    return pl.pallas_call(
        functools.partial(exchange_kernel, cap),
        out_shape=(
            jax.ShapeDtypeStruct((CELLS, LANES), f32),
            jax.ShapeDtypeStruct((32, LANES), f32),
            jax.ShapeDtypeStruct((ROWS, COLS), f32),
            jax.ShapeDtypeStruct((4 * cap, LANES), f32),
            jax.ShapeDtypeStruct((GROUPS, GROUP), i32),
            jax.ShapeDtypeStruct((2 * GROUPS, GROUP), f32),
        ),
        in_specs=[pl.BlockSpec(memory_space=pltpu.HBM)] * 7,
        out_specs=(vmem,) * 6,
        scratch_shapes=[
            pltpu.VMEM((CELLS + 16, LANES), f32),
            pltpu.VMEM((112, LANES), f32),
            pltpu.VMEM((GROUPS, ROWS, LANES), f32),
            pltpu.VMEM((GROUPS, ROWS, LANES), f32),
            pltpu.VMEM((3, GROUPS, GROUP), i32),
            pltpu.SMEM((3, GROUPS, GROUP), i32),
            pltpu.SMEM((2 * GROUPS, GROUP), f32),
            pltpu.VMEM((2, SPEC), f32),
            pltpu.VMEM((1, 256), i32),
            pltpu.VMEM((1, 256), i32),
            pltpu.VMEM((1, 256), f32),
            pltpu.VMEM((1, 256), f32),
            pltpu.VMEM((ROWS, COLS), i32),
            pltpu.VMEM((LON, LANES), f32),
            pltpu.VMEM((DEV, LANES), f32),
            pltpu.VMEM((LANES, DEV), f32),
            pltpu.VMEM((4, NROW, EXT), f32),
            pltpu.VMEM((4, NROW, LANES), f32),
            pltpu.VMEM((4, NROW, LANES), f32),
            pltpu.VMEM((GROUPS, ROWS, LANES), f32),
            pltpu.VMEM((8, NROW, EXT), f32),
            pltpu.VMEM((2 * cap, LANES), f32),
            pltpu.VMEM((2 * cap, LANES), f32),
            pltpu.VMEM((2, lists, LANES), i32),
            pltpu.SMEM((2, lists, LANES), i32),
            pltpu.SemaphoreType.DMA((LOADS,)),
            pltpu.SemaphoreType.DMA((8,)),
            pltpu.SemaphoreType.DMA,
            pltpu.SemaphoreType.DMA((2,)),
            pltpu.SemaphoreType.DMA((2,)),
            pltpu.SemaphoreType.DMA((4,)),
            pltpu.SemaphoreType.DMA((8,)),
            pltpu.SemaphoreType.DMA((4,)),
        ],
        compiler_params=pltpu.CompilerParams(
            collective_id=0 if cap == CAP_HALF else 1,
            has_side_effects=True,
            vmem_limit_bytes=30 * 2**20,
        ),
        name=f"exchange_{cap}",
    )(spectrum, courant, *observed)


def update_kernel(
    partial,
    rim_tables,
    increments,
    rows,
    places,
    speeds,
    out,
    increment,
    stage,
    place,
    speed,
    sems,
    out_sems,
):
    copies = [
        pltpu.make_async_copy(places, place, sems.at[0]),
        pltpu.make_async_copy(speeds, speed, sems.at[1]),
    ]
    for copy in copies:
        copy.start()
    increment[...] = increments[...]
    for copy in copies:
        copy.wait()
    size = GROUP * 16

    def store(group):
        part = pl.ds(pl.multiple_of(group * size, size), size)
        return pltpu.make_async_copy(stage.at[part], out.at[part], out_sems.at[group])

    def finish(step):
        for u in range(GROUP):
            at = (step * GROUP + u) * 16
            slow = jnp.full((ROWS, LANES), speed[GROUPS + step, u])
            down = slow < 0.0
            slow = jnp.abs(slow)
            line = place[step, u]
            for half in range(2):
                first = 8 * half
                way = jnp.where(
                    down,
                    rim_tables[16 + first : 24 + first, :],
                    rim_tables[first : first + 8, :],
                )
                row = jnp.broadcast_to(rows[pl.ds(line + half, 1), :], (ROWS, LANES))
                here = pl.ds(pl.multiple_of(at + first, 8), 8)
                stage[here, :] = partial[here, :] + slow * (row * way)

    finish(0)

    def follow(step, carry):
        finish(step)
        store(step - 1).start()
        return carry

    lax.fori_loop(1, GROUPS, follow, 0)
    store(GROUPS - 1).start()
    lax.fori_loop(0, GROUPS, lambda g, carry: (store(g).wait(), carry)[1], 0)


def update(cap, *sent):
    vmem = pl.BlockSpec(memory_space=pltpu.VMEM)
    return pl.pallas_call(
        update_kernel,
        out_shape=(
            jax.ShapeDtypeStruct((CELLS, LANES), f32),
            jax.ShapeDtypeStruct((ROWS, COLS), f32),
        ),
        in_specs=[vmem] * 6,
        out_specs=(pl.BlockSpec(memory_space=pl.ANY), vmem),
        scratch_shapes=[
            pltpu.VMEM((CELLS, LANES), f32),
            pltpu.SMEM((GROUPS, GROUP), i32),
            pltpu.SMEM((2 * GROUPS, GROUP), f32),
            pltpu.SemaphoreType.DMA((2,)),
            pltpu.SemaphoreType.DMA((GROUPS,)),
        ],
        compiler_params=pltpu.CompilerParams(vmem_limit_bytes=20 * 2**20),
        name=f"update_{cap}",
    )(*sent)


def body(spectrum, sea_mask, courant, obs_tile, obs_cell, obs_value, obs_error):
    halves = spectrum.reshape(SPEC, ROWS, 2, LANES).transpose(0, 2, 1, 3)
    observed = (
        obs_tile.reshape(1, -1),
        obs_cell.reshape(1, -1),
        obs_value.reshape(1, -1),
        obs_error.reshape(1, -1),
        sea_mask,
    )
    over = lax.reduce(
        (courant[1] < 0.0).astype(i32), jnp.int32(CAP_HALF - SPEC), lax.add, (0,)
    )
    fits = over.astype(jnp.uint32) <= 2 * CAP_HALF - SPEC

    def run(cap):
        sent = exchange(cap, halves.reshape(CELLS, LANES), courant, *observed)
        return update(cap, *sent)

    updated, increment = lax.cond(fits, lambda: run(CAP_HALF), lambda: run(CAP_ALL))
    updated = updated.reshape(SPEC, 2, ROWS, LANES).transpose(0, 2, 1, 3)
    return updated.reshape(SPEC, ROWS, COLS), increment


def solution(mesh):
    return jax.shard_map(
        body,
        mesh=mesh,
        in_specs=(
            P(None, "lat", "lon"),
            P("lat", "lon"),
            P(),
            P(("lat", "lon"), None),
            P(("lat", "lon")),
            P(("lat", "lon")),
            P(("lat", "lon")),
        ),
        out_specs=(P(None, "lat", "lon"), P("lat", "lon")),
        check_vma=False,
    )
```

```python
import functools

import jax
import jax.numpy as jnp
from jax import lax
from jax.experimental import pallas as pl
from jax.experimental.pallas import tpu as pltpu
from jax.sharding import PartitionSpec as P

SPEC = 1296
ROWS = 8
COLS = 256
LAT = 4
LON = 32
DEV = LAT * LON
NROW = LAT * ROWS
PASSES = 8
LANES = 128
GROUP = 72
GROUPS = SPEC // GROUP
CELLS = SPEC * 16
LOADS = 6
EXT = 384
RIM = 9
CHUNK = 64
CAP_HALF = 704
CAP_ALL = 1344

spread_rate = 0.2
prior_weight = 4.0

f32 = jnp.float32
i32 = jnp.int32
bf16 = jnp.bfloat16
MESH = pl.DeviceIdType.MESH
LOGICAL = pl.DeviceIdType.LOGICAL
NT = (((1,), (1,)), ((), ()))
NN = (((1,), (0,)), ((), ()))


def thirds(x):
    high = x.astype(bf16)
    rest = x - high.astype(f32)
    mid = rest.astype(bf16)
    low = (rest - mid.astype(f32)).astype(bf16)
    return high, mid, low


def exchange_kernel(
    cap,
    spectrum,
    courant,
    obs_tile,
    obs_cell,
    obs_value,
    obs_error,
    sea,
    partial,
    rim_tables,
    increments,
    rows,
    places,
    own_groups,
    cells,
    tables,
    cols_west,
    cols_east,
    plan,
    steps,
    speeds,
    own_courant,
    own_tile,
    own_cell,
    own_value,
    own_error,
    own_sea,
    outbox,
    inbox,
    turned,
    fields,
    near_west,
    near_east,
    own_edge,
    padded,
    going_north,
    going_south,
    listed,
    picks,
    load_sems,
    small_sems,
    list_sem,
    box_sems,
    lat_sems,
    col_sems,
    rim_sems,
    row_sems,
):
    lat = lax.axis_index("lat")
    lon = lax.axis_index("lon")
    me = lat * LON + lon
    west = lax.rem(lon + LON - 1, LON)
    east = lax.rem(lon + 1, LON)
    chunks = cap // CHUNK

    small = [
        pltpu.make_async_copy(source, target, small_sems.at[number])
        for number, (source, target) in enumerate(
            (
                (obs_tile, own_tile),
                (obs_error, own_error),
                (obs_value, own_value),
                (obs_cell, own_cell),
                (courant, own_courant),
                (sea, own_sea),
            )
        )
    ]
    for copy in small:
        copy.start()
    size = CELLS // LOADS
    loads = [
        pltpu.make_async_copy(
            spectrum.at[pl.ds(part * size, size)],
            cells.at[pl.ds(8 + part * size, size)],
            load_sems.at[part],
        )
        for part in range(LOADS)
    ]
    for copy in loads:
        copy.start()

    barrier = pltpu.get_barrier_semaphore()

    def greet(turn, carry):
        for u in range(7):
            pl.semaphore_signal(
                barrier,
                inc=1,
                device_id=lax.rem(me + (turn * 7 + u + 1), DEV),
                device_id_type=LOGICAL,
            )
        return carry

    lax.fori_loop(0, 18, greet, 0)
    pl.semaphore_signal(
        barrier,
        inc=1,
        device_id=lax.rem(me + DEV - 1, DEV),
        device_id_type=LOGICAL,
    )

    for copy in small[4:6]:
        copy.wait()
    number = lax.broadcasted_iota(i32, (16, LANES), 0) * LANES + lax.broadcasted_iota(
        i32, (16, LANES), 1
    )
    speed = jnp.concatenate(
        [own_courant[1:2, t * LANES : (t + 1) * LANES] for t in range(SPEC // LANES)]
        + [
            jnp.concatenate(
                [
                    own_courant[1:2, SPEC // LANES * LANES : SPEC],
                    jnp.zeros((1, LANES - SPEC % LANES), f32),
                ],
                axis=1,
            )
        ]
        + [jnp.zeros((15 - SPEC // LANES, LANES), f32)],
        axis=0,
    )
    backward = jnp.where(speed < 0.0, 1.0, 0.0).astype(bf16)
    upper = jnp.where(
        lax.broadcasted_iota(i32, (LANES, LANES), 0)
        <= lax.broadcasted_iota(i32, (LANES, LANES), 1),
        1.0,
        0.0,
    ).astype(bf16)
    within = lax.dot_general(backward, upper, NN, preferred_element_type=f32)
    whole = lax.dot_general(
        backward, jnp.ones((LANES, LANES), bf16), NN, preferred_element_type=f32
    )
    lower = jnp.where(
        lax.broadcasted_iota(i32, (16, 16), 1) < lax.broadcasted_iota(i32, (16, 16), 0),
        1.0,
        0.0,
    ).astype(bf16)
    south_upto = within + lax.dot_general(
        lower, whole.astype(bf16), NN, preferred_element_type=f32
    )
    beyond = number >= SPEC
    far = 4.0 * SPEC
    upto = (
        jnp.where(beyond, far, (number + 1).astype(f32) - south_upto),
        jnp.where(beyond, far, south_upto),
    )
    ones = jnp.ones((8, LANES), bf16)

    def enlist(turn, carry):
        place = (
            turn * LANES + lax.broadcasted_iota(i32, (LANES, LANES), 0)
        ).astype(f32)
        for side in range(2):
            count = jnp.zeros((LANES, LANES), f32)
            for t in range(SPEC // LANES + 1):
                count = count + jnp.where(upto[side][t : t + 1, :] <= place, 1.0, 0.0)
            total = lax.dot_general(
                ones, count.astype(bf16), NT, preferred_element_type=f32
            )
            listed[side, pl.ds(turn, 1), :] = jnp.maximum(
                jnp.minimum(total[0:1, :].astype(i32), SPEC - 1), 0
            )
        return carry

    lax.fori_loop(0, listed.shape[1], enlist, 0)
    to_scalars = pltpu.make_async_copy(listed, picks, list_sem)
    to_scalars.start()

    def pick_chunk(number):
        def pick(turn, carry):
            for u in range(8):
                at = number * CHUNK + turn * 8 + u
                line = lax.div(number, 2)
                spot = lax.rem(number, 2) * CHUNK + turn * 8 + u
                first = 8 + 16 * picks[0, line, spot]
                going_north[pl.ds(2 * at, 1), :] = cells[pl.ds(first + 7, 1), :]
                going_north[pl.ds(2 * at + 1, 1), :] = cells[pl.ds(first + 15, 1), :]
                first = 8 + 16 * picks[1, line, spot]
                going_south[pl.ds(2 * at, 1), :] = cells[pl.ds(first, 1), :]
                going_south[pl.ds(2 * at + 1, 1), :] = cells[pl.ds(first + 8, 1), :]
            return carry

        lax.fori_loop(0, CHUNK // 8, pick, 0)

    def north_copy(first, count):
        return pltpu.make_async_remote_copy(
            src_ref=going_north.at[pl.ds(first, count)],
            dst_ref=rows.at[pl.ds(first, count)],
            send_sem=row_sems.at[0],
            recv_sem=row_sems.at[1],
            device_id=(lat + 1, lon),
            device_id_type=MESH,
        )

    def south_copy(first, count):
        return pltpu.make_async_remote_copy(
            src_ref=going_south.at[pl.ds(first, count)],
            dst_ref=rows.at[pl.ds(2 * cap + first, count)],
            send_sem=row_sems.at[2],
            recv_sem=row_sems.at[3],
            device_id=(lat - 1, lon),
            device_id_type=MESH,
        )

    def send_chunk(number):
        first = pl.multiple_of(number * (2 * CHUNK), 2 * CHUNK)

        @pl.when(lat < LAT - 1)
        def _():
            north_copy(first, 2 * CHUNK).start()

        @pl.when(lat > 0)
        def _():
            south_copy(first, 2 * CHUNK).start()

    for copy in loads:
        copy.wait()
    to_scalars.wait()
    pick_chunk(0)
    pick_chunk(1)
    pick_chunk(2)
    pl.semaphore_wait(barrier, DEV - 1)
    for number in range(3):
        send_chunk(number)

    for copy in small[0:4]:
        copy.wait()
    owner = own_tile[...]
    owner_lat = lax.shift_right_logical(owner, 5)
    owner_lon = lax.bitwise_and(owner, 31)
    tiles = lax.broadcasted_iota(i32, (DEV, 256), 0)
    hit = jnp.where(tiles == owner, 1.0, 0.0)
    before = jnp.where(
        lax.broadcasted_iota(i32, (256, 256), 0)
        < lax.broadcasted_iota(i32, (256, 256), 1),
        1.0,
        0.0,
    )
    earlier = lax.dot_general(
        hit.astype(bf16), before.astype(bf16), NN, preferred_element_type=f32
    )
    rank = jnp.sum(hit * earlier, axis=0, keepdims=True).astype(i32)
    slot = owner_lat * 8 + rank
    slots = lax.broadcasted_iota(i32, (32, 256), 0)
    in_slot = slots == slot
    to_lon = jnp.where(slots == owner_lon, 1.0, 0.0).astype(bf16)
    zero = jnp.zeros((32, 256), f32)
    weights = 1.0 / own_error[...]
    spread = jnp.concatenate(
        [
            jnp.where(in_slot, value, zero)
            for value in (weights * own_value[...], weights, own_cell[...].astype(f32))
        ]
        + [zero],
        axis=0,
    )
    packed = jnp.zeros((LON, LANES), f32)
    for piece in thirds(spread):
        packed = packed + lax.dot_general(
            to_lon, piece, NT, preferred_element_type=f32
        )
    outbox[...] = packed

    def post(turn, carry):
        for u in range(7):
            peer = lax.rem(me + (turn * 7 + u + 1), DEV)
            post_to(peer)
        return carry

    def post_to(peer):
        pltpu.make_async_remote_copy(
            src_ref=outbox.at[pl.ds(lax.rem(peer, LON), 1)],
            dst_ref=inbox.at[pl.ds(me, 1)],
            send_sem=box_sems.at[0],
            recv_sem=box_sems.at[1],
            device_id=peer,
            device_id_type=LOGICAL,
        ).start()

    lax.fori_loop(0, 18, post, 0)
    post_to(lax.rem(me + DEV - 1, DEV))
    inbox[pl.ds(me, 1), :] = outbox[pl.ds(lon, 1), :]

    for group in range(GROUPS):
        for way in range(2):
            own_groups[way * GROUPS + group : way * GROUPS + group + 1, :] = own_courant[
                way : way + 1, group * GROUP : (group + 1) * GROUP
            ]
    to_east = own_groups[0:GROUPS, :] < 0.0
    to_north = own_groups[GROUPS : 2 * GROUPS, :] < 0.0
    shape = (GROUPS, GROUP)
    group = lax.broadcasted_iota(i32, shape, 0)
    member = lax.broadcasted_iota(i32, shape, 1)
    number = group * GROUP + member
    backward = jnp.where(to_north, 1.0, 0.0).astype(bf16)
    upper = jnp.where(
        lax.broadcasted_iota(i32, (GROUP, GROUP), 0)
        < lax.broadcasted_iota(i32, (GROUP, GROUP), 1),
        1.0,
        0.0,
    ).astype(bf16)
    whole = lax.dot_general(
        backward, jnp.ones((GROUP, GROUP), bf16), NN, preferred_element_type=f32
    )
    lower = jnp.where(
        lax.broadcasted_iota(i32, (GROUPS, GROUPS), 1)
        < lax.broadcasted_iota(i32, (GROUPS, GROUPS), 0),
        1.0,
        0.0,
    ).astype(bf16)
    south = (
        lax.dot_general(backward, upper, NN, preferred_element_type=f32)
        + lax.dot_general(lower, whole.astype(bf16), NN, preferred_element_type=f32)
    ).astype(i32)
    plan[0] = jnp.where(to_east, LANES - 1, 1)
    plan[1] = jnp.where(
        to_east, LANES - 1 - member, jnp.where(member == 0, 0, LANES - member)
    )
    plan[2] = 8 + 16 * number + jnp.where(to_north, 1, -1)
    places[...] = 2 * jnp.where(to_north, cap + south, number - south)
    scalars = [
        pltpu.make_async_copy(plan, steps, small_sems.at[6]),
        pltpu.make_async_copy(own_groups, speeds, small_sems.at[7]),
    ]
    for copy in scalars:
        copy.start()
    cells[0:8, :] = jnp.zeros((8, LANES), f32)
    cells[8 + CELLS : 16 + CELLS, :] = jnp.zeros((8, LANES), f32)

    for copy in scalars:
        copy.wait()

    lane = lax.broadcasted_iota(i32, (ROWS, LANES), 1)
    blank = jnp.zeros((ROWS, LANES), f32)

    def gather(pair, sums):
        sums = list(sums)
        for half in range(2):
            group = 2 * pair + half
            edge = blank
            for u in range(GROUP):
                at = 8 + (group * GROUP + u) * 16
                left = cells[pl.ds(pl.multiple_of(at, 8), ROWS), :]
                right = cells[pl.ds(pl.multiple_of(at + 8, 8), ROWS), :]
                k = 2 * (u % 4)
                sums[k] = sums[k] + left
                sums[k + 1] = sums[k + 1] + right
                speed = speeds[group, u]
                taken = jnp.where(jnp.full((ROWS, LANES), speed) < 0.0, left, right)
                turn = jnp.where(speed < 0.0, u, u + 1)
                edge = jnp.where(lane == u, pltpu.roll(taken, turn, 1), edge)
            own_edge[group] = edge
        return tuple(sums)

    sums = lax.fori_loop(0, GROUPS // 2, gather, tuple(blank for _ in range(8)))
    left = (sums[0] + sums[2]) + (sums[4] + sums[6])
    right = (sums[1] + sums[3]) + (sums[5] + sums[7])
    here_rows = pl.ds(pl.multiple_of(lat * ROWS, ROWS), ROWS)
    fields[2, here_rows, 0:LANES] = 4.0 * jnp.sqrt(left / SPEC)
    fields[2, here_rows, LANES:COLS] = 4.0 * jnp.sqrt(right / SPEC)
    fields[3, here_rows, 0:COLS] = own_sea[...].astype(f32)

    for step in range(1, LAT):
        peer = lax.rem(lat + step, LAT)
        part = fields.at[pl.ds(2, 2), here_rows, pl.ds(0, COLS)]
        pltpu.make_async_remote_copy(
            src_ref=part,
            dst_ref=part,
            send_sem=lat_sems.at[0],
            recv_sem=lat_sems.at[1],
            device_id=(peer, lon),
            device_id_type=MESH,
        ).start()

    send_west = pltpu.make_async_remote_copy(
        src_ref=own_edge,
        dst_ref=cols_east,
        send_sem=col_sems.at[0],
        recv_sem=col_sems.at[1],
        device_id=(lat, west),
        device_id_type=MESH,
    )
    send_east = pltpu.make_async_remote_copy(
        src_ref=own_edge,
        dst_ref=cols_west,
        send_sem=col_sems.at[2],
        recv_sem=col_sems.at[3],
        device_id=(lat, east),
        device_id_type=MESH,
    )
    send_west.start()
    send_east.start()

    pick_chunk(3)

    def forward(number, carry):
        pick_chunk(number)
        send_chunk(number - 1)
        return carry

    early = chunks * 7 // 11
    lax.fori_loop(4, early, forward, 0)

    @pl.when(lat == 0)
    def _():
        rows[0 : 2 * cap, :] = jnp.zeros((2 * cap, LANES), f32)

    @pl.when(lat == LAT - 1)
    def _():
        rows[2 * cap : 4 * cap, :] = jnp.zeros((2 * cap, LANES), f32)

    def rim_copies(first, sems):
        part = pl.ds(first, 2)
        return (
            pltpu.make_async_remote_copy(
                src_ref=fields.at[part, pl.ds(0, NROW), pl.ds(0, LANES)],
                dst_ref=near_east.at[part],
                send_sem=rim_sems.at[sems],
                recv_sem=rim_sems.at[sems + 1],
                device_id=(lat, west),
                device_id_type=MESH,
            ),
            pltpu.make_async_remote_copy(
                src_ref=fields.at[part, pl.ds(0, NROW), pl.ds(LANES, LANES)],
                dst_ref=near_west.at[part],
                send_sem=rim_sems.at[sems + 2],
                recv_sem=rim_sems.at[sems + 3],
                device_id=(lat, east),
                device_id_type=MESH,
            ),
        )

    got = pl.ds(0, DEV - 1)
    pltpu.make_async_copy(inbox.at[got], inbox.at[got], box_sems.at[1]).wait()
    turned[...] = inbox[...].T

    def place(number, carry):
        base = pl.multiple_of(number * 8, 8)
        misfits = turned[pl.ds(base, 8), :]
        weights = turned[pl.ds(base + 32, 8), :]
        cell = turned[pl.ds(base + 64, 8), :].astype(i32)
        cell_row = lax.shift_right_logical(cell, 8)
        cell_col = lax.bitwise_and(cell, 255)
        rows8 = lax.broadcasted_iota(i32, (8, LANES), 0)
        cols = lax.broadcasted_iota(i32, (COLS, LANES), 0)
        spots, sent = [], []
        for s in range(8):
            spots.append(jnp.where(cols == cell_col[s : s + 1, :], 1.0, 0.0).astype(bf16))
            at_row = rows8 == cell_row[s : s + 1, :]
            sent.append(
                jnp.concatenate(
                    [
                        jnp.where(at_row, misfits[s : s + 1, :], 0.0),
                        jnp.where(at_row, weights[s : s + 1, :], 0.0),
                    ],
                    axis=0,
                )
            )
        spots = jnp.concatenate(spots, axis=1)
        sent = jnp.concatenate(sent, axis=1)
        total = lax.dot_general(
            jnp.concatenate(thirds(sent), axis=0), spots, NT, preferred_element_type=f32
        )
        total = total[0:16, :] + total[16:32, :] + total[32:48, :]
        fields[0, pl.ds(base, 8), 0:COLS] = total[0:8, :]
        fields[1, pl.ds(base, 8), 0:COLS] = total[8:16, :]
        return carry

    lax.fori_loop(0, LAT, place, 0)

    three = fields.at[pl.ds(2, 2), pl.ds(0, NROW - ROWS), pl.ds(0, COLS)]
    pltpu.make_async_copy(three, three, lat_sems.at[1]).wait()
    pltpu.make_async_copy(three, three, lat_sems.at[0]).wait()
    coast_rims = rim_copies(2, 0)
    for copy in coast_rims:
        copy.start()
    height = fields[2, :, 0:COLS]
    ocean = fields[3, :, 0:COLS]
    weight = fields[1, :, 0:COLS] * ocean
    fields[0, :, 0:COLS] = (fields[0, :, 0:COLS] - height * fields[1, :, 0:COLS]) * ocean
    fields[1, :, 0:COLS] = weight
    field_rims = rim_copies(0, 4)
    for copy in field_rims:
        copy.start()
    lax.fori_loop(early, chunks, forward, 0)
    send_chunk(chunks - 1)
    for copy in coast_rims + field_rims:
        copy.wait()
    lane = lax.broadcasted_iota(i32, (NROW, LANES), 1)
    for number, filler in enumerate((0.0, 0.0, 1.0, 0.0)):
        fields[number, :, COLS:EXT] = jnp.where(
            lane < RIM,
            near_east[number],
            jnp.where(lane >= LANES - RIM, near_west[number], filler),
        )

    row = lax.broadcasted_iota(i32, (NROW, EXT), 0)

    def north_of(x):
        return jnp.where(row == NROW - 1, 0.0, pltpu.roll(x, NROW - 1, 0))

    def south_of(x):
        return jnp.where(row == 0, 0.0, pltpu.roll(x, 1, 0))

    def east_of(x):
        return pltpu.roll(x, EXT - 1, 1)

    def west_of(x):
        return pltpu.roll(x, 1, 1)

    ocean = fields[3]
    share = spread_rate * ocean
    keep = 1.0 - share * (
        north_of(ocean) + south_of(ocean) + east_of(ocean) + west_of(ocean)
    )

    def relax(x):
        return keep * x + share * (
            (north_of(x) + south_of(x)) + (east_of(x) + west_of(x))
        )

    def relax_both(_, pair):
        return relax(pair[0]), relax(pair[1])

    misfit, weight = lax.fori_loop(0, PASSES, relax_both, (fields[0], fields[1]))
    increment = ocean * misfit / (prior_weight + weight)
    factor = jnp.exp(2.0 * increment / fields[2]) * ocean
    going_up = factor * north_of(ocean)
    going_down = factor * south_of(ocean)
    for number, value in enumerate(
        (
            factor,
            factor * east_of(ocean),
            factor * west_of(ocean),
            going_up,
            going_down,
            south_of(going_up),
            north_of(going_down),
            increment,
        )
    ):
        padded[number] = value
    own = here_rows
    sub = lax.broadcasted_iota(i32, (ROWS, LANES), 0)
    for number in range(7):
        for half in range(2):
            value = padded[number, own, half * LANES : (half + 1) * LANES]
            if number == 5:
                rim_tables[8 * half : 8 * half + 8, :] = jnp.where(sub == 0, value, 0.0)
                value = jnp.where(sub == 0, 0.0, value)
            if number == 6:
                outer = sub == ROWS - 1
                rim_tables[16 + 8 * half : 24 + 8 * half, :] = jnp.where(
                    outer, value, 0.0
                )
                value = jnp.where(outer, 0.0, value)
            tables[16 * number + 8 * half : 16 * number + 8 * half + 8, :] = value
    increments[...] = padded[7, own, 0:COLS]
    beside = (
        jnp.broadcast_to(padded[1, own, EXT - 1 : EXT], (ROWS, LANES)),
        jnp.broadcast_to(padded[2, own, COLS : COLS + 1], (ROWS, LANES)),
    )

    send_west.wait()
    send_east.wait()

    def advance(step, carry):
        rims = cols_west[step] * beside[0], cols_east[step] * beside[1]
        for u in range(GROUP):
            at = 8 + (step * GROUP + u) * 16
            near = steps[2, step, u]
            speed = jnp.full((ROWS, LANES), speeds[step, u])
            back = speed < 0.0
            cell, flow = [], []
            for half in range(2):
                first = 8 * half
                cell.append(cells[pl.ds(pl.multiple_of(at + first, 8), 8), :])
                way = jnp.where(
                    back, tables[32 + first : 40 + first, :], tables[16 + first : 24 + first, :]
                )
                flow.append(cell[half] * way)
            shift = steps[0, step, u]
            moved = pltpu.roll(flow[0], shift, 1), pltpu.roll(flow[1], shift, 1)
            rim = pltpu.roll(jnp.where(back, rims[1], rims[0]), steps[1, step, u], 1)
            at_edge = lane == jnp.where(back, LANES - 1, 0)
            came = (
                jnp.where(at_edge, jnp.where(back, moved[1], rim), moved[0]),
                jnp.where(at_edge, jnp.where(back, rim, moved[0]), moved[1]),
            )
            speed = jnp.abs(speed)
            slow = jnp.full((ROWS, LANES), speeds[GROUPS + step, u])
            down = slow < 0.0
            slow = jnp.abs(slow)
            for half in range(2):
                first = 8 * half
                way = jnp.where(
                    down, tables[64 + first : 72 + first, :], tables[48 + first : 56 + first, :]
                )
                way_in = jnp.where(
                    down, tables[96 + first : 104 + first, :], tables[80 + first : 88 + first, :]
                )
                gone = cell[half] * way - cells[pl.ds(near + first, 8), :] * way_in
                to = pl.multiple_of((step * GROUP + u) * 16 + first, 8)
                partial[pl.ds(to, 8), :] = (
                    cell[half] * tables[first : first + 8, :]
                    - speed * (flow[half] - came[half])
                    - slow * gone
                )
        return carry

    lane = lax.broadcasted_iota(i32, (ROWS, LANES), 1)
    lax.fori_loop(0, GROUPS, advance, 0)

    pltpu.make_async_copy(inbox.at[got], inbox.at[got], box_sems.at[0]).wait()

    @pl.when(lat < LAT - 1)
    def _():
        north_copy(0, 2 * cap).wait_send()
        part = rows.at[pl.ds(2 * cap, 2 * cap)]
        pltpu.make_async_copy(part, part, row_sems.at[3]).wait()

    @pl.when(lat > 0)
    def _():
        south_copy(0, 2 * cap).wait_send()
        part = rows.at[pl.ds(0, 2 * cap)]
        pltpu.make_async_copy(part, part, row_sems.at[1]).wait()


def exchange(cap, spectrum, courant, *observed):
    vmem = pl.BlockSpec(memory_space=pltpu.VMEM)
    lists = -(-cap // LANES)
    return pl.pallas_call(
        functools.partial(exchange_kernel, cap),
        out_shape=(
            jax.ShapeDtypeStruct((CELLS, LANES), f32),
            jax.ShapeDtypeStruct((32, LANES), f32),
            jax.ShapeDtypeStruct((ROWS, COLS), f32),
            jax.ShapeDtypeStruct((4 * cap, LANES), f32),
            jax.ShapeDtypeStruct((GROUPS, GROUP), i32),
            jax.ShapeDtypeStruct((2 * GROUPS, GROUP), f32),
        ),
        in_specs=[pl.BlockSpec(memory_space=pltpu.HBM)] * 7,
        out_specs=(vmem,) * 6,
        scratch_shapes=[
            pltpu.VMEM((CELLS + 16, LANES), f32),
            pltpu.VMEM((112, LANES), f32),
            pltpu.VMEM((GROUPS, ROWS, LANES), f32),
            pltpu.VMEM((GROUPS, ROWS, LANES), f32),
            pltpu.VMEM((3, GROUPS, GROUP), i32),
            pltpu.SMEM((3, GROUPS, GROUP), i32),
            pltpu.SMEM((2 * GROUPS, GROUP), f32),
            pltpu.VMEM((2, SPEC), f32),
            pltpu.VMEM((1, 256), i32),
            pltpu.VMEM((1, 256), i32),
            pltpu.VMEM((1, 256), f32),
            pltpu.VMEM((1, 256), f32),
            pltpu.VMEM((ROWS, COLS), i32),
            pltpu.VMEM((LON, LANES), f32),
            pltpu.VMEM((DEV, LANES), f32),
            pltpu.VMEM((LANES, DEV), f32),
            pltpu.VMEM((4, NROW, EXT), f32),
            pltpu.VMEM((4, NROW, LANES), f32),
            pltpu.VMEM((4, NROW, LANES), f32),
            pltpu.VMEM((GROUPS, ROWS, LANES), f32),
            pltpu.VMEM((8, NROW, EXT), f32),
            pltpu.VMEM((2 * cap, LANES), f32),
            pltpu.VMEM((2 * cap, LANES), f32),
            pltpu.VMEM((2, lists, LANES), i32),
            pltpu.SMEM((2, lists, LANES), i32),
            pltpu.SemaphoreType.DMA((LOADS,)),
            pltpu.SemaphoreType.DMA((8,)),
            pltpu.SemaphoreType.DMA,
            pltpu.SemaphoreType.DMA((2,)),
            pltpu.SemaphoreType.DMA((2,)),
            pltpu.SemaphoreType.DMA((4,)),
            pltpu.SemaphoreType.DMA((8,)),
            pltpu.SemaphoreType.DMA((4,)),
        ],
        compiler_params=pltpu.CompilerParams(
            collective_id=0 if cap == CAP_HALF else 1,
            has_side_effects=True,
            vmem_limit_bytes=30 * 2**20,
        ),
        name=f"exchange_{cap}",
    )(spectrum, courant, *observed)


def update_kernel(
    partial,
    rim_tables,
    increments,
    rows,
    places,
    speeds,
    out,
    increment,
    stage,
    place,
    speed,
    sems,
    out_sems,
):
    copies = [
        pltpu.make_async_copy(places, place, sems.at[0]),
        pltpu.make_async_copy(speeds, speed, sems.at[1]),
    ]
    for copy in copies:
        copy.start()
    increment[...] = increments[...]
    for copy in copies:
        copy.wait()
    size = GROUP * 16

    def store(group):
        part = pl.ds(pl.multiple_of(group * size, size), size)
        return pltpu.make_async_copy(stage.at[part], out.at[part], out_sems.at[group])

    def finish(step):
        for u in range(GROUP):
            at = (step * GROUP + u) * 16
            slow = jnp.full((ROWS, LANES), speed[GROUPS + step, u])
            down = slow < 0.0
            slow = jnp.abs(slow)
            line = place[step, u]
            for half in range(2):
                first = 8 * half
                way = jnp.where(
                    down,
                    rim_tables[16 + first : 24 + first, :],
                    rim_tables[first : first + 8, :],
                )
                row = jnp.broadcast_to(rows[pl.ds(line + half, 1), :], (ROWS, LANES))
                here = pl.ds(pl.multiple_of(at + first, 8), 8)
                stage[here, :] = partial[here, :] + slow * (row * way)

    finish(0)

    def follow(step, carry):
        finish(step)
        store(step - 1).start()
        return carry

    lax.fori_loop(1, GROUPS, follow, 0)
    store(GROUPS - 1).start()
    lax.fori_loop(0, GROUPS, lambda g, carry: (store(g).wait(), carry)[1], 0)


def update(cap, *sent):
    vmem = pl.BlockSpec(memory_space=pltpu.VMEM)
    return pl.pallas_call(
        update_kernel,
        out_shape=(
            jax.ShapeDtypeStruct((CELLS, LANES), f32),
            jax.ShapeDtypeStruct((ROWS, COLS), f32),
        ),
        in_specs=[vmem] * 6,
        out_specs=(pl.BlockSpec(memory_space=pl.ANY), vmem),
        scratch_shapes=[
            pltpu.VMEM((CELLS, LANES), f32),
            pltpu.SMEM((GROUPS, GROUP), i32),
            pltpu.SMEM((2 * GROUPS, GROUP), f32),
            pltpu.SemaphoreType.DMA((2,)),
            pltpu.SemaphoreType.DMA((GROUPS,)),
        ],
        compiler_params=pltpu.CompilerParams(vmem_limit_bytes=20 * 2**20),
        name=f"update_{cap}",
    )(*sent)


def body(spectrum, sea_mask, courant, obs_tile, obs_cell, obs_value, obs_error):
    halves = spectrum.reshape(SPEC, ROWS, 2, LANES).transpose(0, 2, 1, 3)
    observed = (
        obs_tile.reshape(1, -1),
        obs_cell.reshape(1, -1),
        obs_value.reshape(1, -1),
        obs_error.reshape(1, -1),
        sea_mask,
    )
    over = jnp.sum((courant[1] < 0.0).astype(i32)) - (SPEC - CAP_HALF)
    fits = over.astype(jnp.uint32) <= 2 * CAP_HALF - SPEC

    def run(cap):
        sent = exchange(cap, halves.reshape(CELLS, LANES), courant, *observed)
        return update(cap, *sent)

    updated, increment = lax.cond(fits, lambda: run(CAP_HALF), lambda: run(CAP_ALL))
    updated = updated.reshape(SPEC, 2, ROWS, LANES).transpose(0, 2, 1, 3)
    return updated.reshape(SPEC, ROWS, COLS), increment


def solution(mesh):
    return jax.shard_map(
        body,
        mesh=mesh,
        in_specs=(
            P(None, "lat", "lon"),
            P("lat", "lon"),
            P(),
            P(("lat", "lon"), None),
            P(("lat", "lon")),
            P(("lat", "lon")),
            P(("lat", "lon")),
        ),
        out_specs=(P(None, "lat", "lon"), P("lat", "lon")),
        check_vma=False,
    )
```

```python
import functools

import jax
import jax.numpy as jnp
from jax import lax
from jax.experimental import pallas as pl
from jax.experimental.pallas import tpu as pltpu
from jax.sharding import PartitionSpec as P

SPEC = 1296
ROWS = 8
COLS = 256
LAT = 4
LON = 32
DEV = LAT * LON
NROW = LAT * ROWS
PASSES = 8
LANES = 128
GROUP = 72
GROUPS = SPEC // GROUP
CELLS = SPEC * 16
LOADS = 6
EXT = 384
RIM = 9
CHUNK = 64
CAP_HALF = 704
CAP_ALL = 1344

spread_rate = 0.2
prior_weight = 4.0

f32 = jnp.float32
i32 = jnp.int32
bf16 = jnp.bfloat16
MESH = pl.DeviceIdType.MESH
LOGICAL = pl.DeviceIdType.LOGICAL
NT = (((1,), (1,)), ((), ()))
NN = (((1,), (0,)), ((), ()))


def thirds(x):
    high = x.astype(bf16)
    rest = x - high.astype(f32)
    mid = rest.astype(bf16)
    low = (rest - mid.astype(f32)).astype(bf16)
    return high, mid, low


def exchange_kernel(
    cap,
    spectrum,
    courant,
    obs_tile,
    obs_cell,
    obs_value,
    obs_error,
    sea,
    partial,
    rim_tables,
    increments,
    rows,
    places,
    own_groups,
    cells,
    tables,
    cols_west,
    cols_east,
    plan,
    steps,
    speeds,
    own_courant,
    own_tile,
    own_cell,
    own_value,
    own_error,
    own_sea,
    outbox,
    inbox,
    turned,
    fields,
    near_west,
    near_east,
    own_edge,
    padded,
    going_north,
    going_south,
    listed,
    picks,
    load_sems,
    small_sems,
    list_sem,
    box_sems,
    lat_sems,
    col_sems,
    rim_sems,
    row_sems,
):
    lat = lax.axis_index("lat")
    lon = lax.axis_index("lon")
    me = lat * LON + lon
    west = lax.rem(lon + LON - 1, LON)
    east = lax.rem(lon + 1, LON)
    chunks = cap // CHUNK

    small = [
        pltpu.make_async_copy(source, target, small_sems.at[number])
        for number, (source, target) in enumerate(
            (
                (obs_tile, own_tile),
                (obs_error, own_error),
                (obs_value, own_value),
                (obs_cell, own_cell),
                (courant, own_courant),
                (sea, own_sea),
            )
        )
    ]
    for copy in small:
        copy.start()
    size = CELLS // LOADS
    loads = [
        pltpu.make_async_copy(
            spectrum.at[pl.ds(part * size, size)],
            cells.at[pl.ds(8 + part * size, size)],
            load_sems.at[part],
        )
        for part in range(LOADS)
    ]
    for copy in loads:
        copy.start()

    barrier = pltpu.get_barrier_semaphore()

    def greet(turn, carry):
        for u in range(7):
            pl.semaphore_signal(
                barrier,
                inc=1,
                device_id=lax.rem(me + (turn * 7 + u + 1), DEV),
                device_id_type=LOGICAL,
            )
        return carry

    lax.fori_loop(0, 18, greet, 0)
    pl.semaphore_signal(
        barrier,
        inc=1,
        device_id=lax.rem(me + DEV - 1, DEV),
        device_id_type=LOGICAL,
    )

    for copy in small[0:4]:
        copy.wait()
    owner = own_tile[...]
    owner_lat = lax.shift_right_logical(owner, 5)
    owner_lon = lax.bitwise_and(owner, 31)
    tiles = lax.broadcasted_iota(i32, (DEV, 256), 0)
    hit = jnp.where(tiles == owner, 1.0, 0.0)
    before = jnp.where(
        lax.broadcasted_iota(i32, (256, 256), 0)
        < lax.broadcasted_iota(i32, (256, 256), 1),
        1.0,
        0.0,
    )
    earlier = lax.dot_general(
        hit.astype(bf16), before.astype(bf16), NN, preferred_element_type=f32
    )
    rank = jnp.sum(hit * earlier, axis=0, keepdims=True).astype(i32)
    slot = owner_lat * 8 + rank
    slots = lax.broadcasted_iota(i32, (32, 256), 0)
    in_slot = slots == slot
    to_lon = jnp.where(slots == owner_lon, 1.0, 0.0).astype(bf16)
    zero = jnp.zeros((32, 256), f32)
    weights = 1.0 / own_error[...]
    spread = jnp.concatenate(
        [
            jnp.where(in_slot, value, zero)
            for value in (weights * own_value[...], weights, own_cell[...].astype(f32))
        ]
        + [zero],
        axis=0,
    )
    packed = jnp.zeros((LON, LANES), f32)
    for piece in thirds(spread):
        packed = packed + lax.dot_general(
            to_lon, piece, NT, preferred_element_type=f32
        )
    outbox[...] = packed

    for copy in small[4:6]:
        copy.wait()
    for group in range(GROUPS):
        for way in range(2):
            own_groups[way * GROUPS + group : way * GROUPS + group + 1, :] = own_courant[
                way : way + 1, group * GROUP : (group + 1) * GROUP
            ]
    number = lax.broadcasted_iota(i32, (16, LANES), 0) * LANES + lax.broadcasted_iota(
        i32, (16, LANES), 1
    )
    speed = jnp.concatenate(
        [own_courant[1:2, t * LANES : (t + 1) * LANES] for t in range(SPEC // LANES)]
        + [
            jnp.concatenate(
                [
                    own_courant[1:2, SPEC // LANES * LANES : SPEC],
                    jnp.zeros((1, LANES - SPEC % LANES), f32),
                ],
                axis=1,
            )
        ]
        + [jnp.zeros((15 - SPEC // LANES, LANES), f32)],
        axis=0,
    )
    backward = jnp.where(speed < 0.0, 1.0, 0.0).astype(bf16)
    upper = jnp.where(
        lax.broadcasted_iota(i32, (LANES, LANES), 0)
        <= lax.broadcasted_iota(i32, (LANES, LANES), 1),
        1.0,
        0.0,
    ).astype(bf16)
    within = lax.dot_general(backward, upper, NN, preferred_element_type=f32)
    whole = lax.dot_general(
        backward, jnp.ones((LANES, LANES), bf16), NN, preferred_element_type=f32
    )
    lower = jnp.where(
        lax.broadcasted_iota(i32, (16, 16), 1) < lax.broadcasted_iota(i32, (16, 16), 0),
        1.0,
        0.0,
    ).astype(bf16)
    south_upto = within + lax.dot_general(
        lower, whole.astype(bf16), NN, preferred_element_type=f32
    )
    beyond = number >= SPEC
    far = 4.0 * SPEC
    upto = (
        jnp.where(beyond, far, (number + 1).astype(f32) - south_upto),
        jnp.where(beyond, far, south_upto),
    )
    ones = jnp.ones((8, LANES), bf16)

    def enlist(turn, carry):
        place = (
            turn * LANES + lax.broadcasted_iota(i32, (LANES, LANES), 0)
        ).astype(f32)
        for side in range(2):
            count = jnp.zeros((LANES, LANES), f32)
            for t in range(SPEC // LANES + 1):
                count = count + jnp.where(upto[side][t : t + 1, :] <= place, 1.0, 0.0)
            total = lax.dot_general(
                ones, count.astype(bf16), NT, preferred_element_type=f32
            )
            listed[side, pl.ds(turn, 1), :] = jnp.maximum(
                jnp.minimum(total[0:1, :].astype(i32), SPEC - 1), 0
            )
        return carry

    lax.fori_loop(0, listed.shape[1], enlist, 0)
    to_scalars = pltpu.make_async_copy(listed, picks, list_sem)
    to_scalars.start()

    to_east = own_groups[0:GROUPS, :] < 0.0
    to_north = own_groups[GROUPS : 2 * GROUPS, :] < 0.0
    shape = (GROUPS, GROUP)
    group = lax.broadcasted_iota(i32, shape, 0)
    member = lax.broadcasted_iota(i32, shape, 1)
    number = group * GROUP + member
    backward = jnp.where(to_north, 1.0, 0.0).astype(bf16)
    upper = jnp.where(
        lax.broadcasted_iota(i32, (GROUP, GROUP), 0)
        < lax.broadcasted_iota(i32, (GROUP, GROUP), 1),
        1.0,
        0.0,
    ).astype(bf16)
    whole = lax.dot_general(
        backward, jnp.ones((GROUP, GROUP), bf16), NN, preferred_element_type=f32
    )
    lower = jnp.where(
        lax.broadcasted_iota(i32, (GROUPS, GROUPS), 1)
        < lax.broadcasted_iota(i32, (GROUPS, GROUPS), 0),
        1.0,
        0.0,
    ).astype(bf16)
    south = (
        lax.dot_general(backward, upper, NN, preferred_element_type=f32)
        + lax.dot_general(lower, whole.astype(bf16), NN, preferred_element_type=f32)
    ).astype(i32)
    plan[0] = jnp.where(to_east, LANES - 1, 1)
    plan[1] = jnp.where(
        to_east, LANES - 1 - member, jnp.where(member == 0, 0, LANES - member)
    )
    plan[2] = 8 + 16 * number + jnp.where(to_north, 1, -1)
    places[...] = 2 * jnp.where(to_north, cap + south, number - south)
    scalars = [
        pltpu.make_async_copy(plan, steps, small_sems.at[6]),
        pltpu.make_async_copy(own_groups, speeds, small_sems.at[7]),
    ]
    for copy in scalars:
        copy.start()
    cells[0:8, :] = jnp.zeros((8, LANES), f32)
    cells[8 + CELLS : 16 + CELLS, :] = jnp.zeros((8, LANES), f32)

    def pick_chunk(number):
        def pick(turn, carry):
            for u in range(8):
                at = number * CHUNK + turn * 8 + u
                line = lax.div(number, 2)
                spot = lax.rem(number, 2) * CHUNK + turn * 8 + u
                first = 8 + 16 * picks[0, line, spot]
                going_north[pl.ds(2 * at, 1), :] = cells[pl.ds(first + 7, 1), :]
                going_north[pl.ds(2 * at + 1, 1), :] = cells[pl.ds(first + 15, 1), :]
                first = 8 + 16 * picks[1, line, spot]
                going_south[pl.ds(2 * at, 1), :] = cells[pl.ds(first, 1), :]
                going_south[pl.ds(2 * at + 1, 1), :] = cells[pl.ds(first + 8, 1), :]
            return carry

        lax.fori_loop(0, CHUNK // 8, pick, 0)

    def north_copy(first, count):
        return pltpu.make_async_remote_copy(
            src_ref=going_north.at[pl.ds(first, count)],
            dst_ref=rows.at[pl.ds(first, count)],
            send_sem=row_sems.at[0],
            recv_sem=row_sems.at[1],
            device_id=(lat + 1, lon),
            device_id_type=MESH,
        )

    def south_copy(first, count):
        return pltpu.make_async_remote_copy(
            src_ref=going_south.at[pl.ds(first, count)],
            dst_ref=rows.at[pl.ds(2 * cap + first, count)],
            send_sem=row_sems.at[2],
            recv_sem=row_sems.at[3],
            device_id=(lat - 1, lon),
            device_id_type=MESH,
        )

    def send_chunk(number):
        first = pl.multiple_of(number * (2 * CHUNK), 2 * CHUNK)

        @pl.when(lat < LAT - 1)
        def _():
            north_copy(first, 2 * CHUNK).start()

        @pl.when(lat > 0)
        def _():
            south_copy(first, 2 * CHUNK).start()

    pl.semaphore_wait(barrier, DEV - 1)
    def post(turn, carry):
        for u in range(7):
            peer = lax.rem(me + (turn * 7 + u + 1), DEV)
            post_to(peer)
        return carry

    def post_to(peer):
        pltpu.make_async_remote_copy(
            src_ref=outbox.at[pl.ds(lax.rem(peer, LON), 1)],
            dst_ref=inbox.at[pl.ds(me, 1)],
            send_sem=box_sems.at[0],
            recv_sem=box_sems.at[1],
            device_id=peer,
            device_id_type=LOGICAL,
        ).start()

    lax.fori_loop(0, 18, post, 0)
    post_to(lax.rem(me + DEV - 1, DEV))
    inbox[pl.ds(me, 1), :] = outbox[pl.ds(lon, 1), :]

    for copy in loads:
        copy.wait()
    to_scalars.wait()
    for copy in scalars:
        copy.wait()
    pick_chunk(0)
    pick_chunk(1)
    send_chunk(0)
    send_chunk(1)

    lane = lax.broadcasted_iota(i32, (ROWS, LANES), 1)
    blank = jnp.zeros((ROWS, LANES), f32)

    def gather(pair, sums):
        sums = list(sums)
        for half in range(2):
            group = 2 * pair + half
            edge = blank
            for u in range(GROUP):
                at = 8 + (group * GROUP + u) * 16
                left = cells[pl.ds(pl.multiple_of(at, 8), ROWS), :]
                right = cells[pl.ds(pl.multiple_of(at + 8, 8), ROWS), :]
                k = 2 * (u % 4)
                sums[k] = sums[k] + left
                sums[k + 1] = sums[k + 1] + right
                speed = speeds[group, u]
                taken = jnp.where(jnp.full((ROWS, LANES), speed) < 0.0, left, right)
                turn = jnp.where(speed < 0.0, u, u + 1)
                edge = jnp.where(lane == u, pltpu.roll(taken, turn, 1), edge)
            own_edge[group] = edge
        return tuple(sums)

    sums = lax.fori_loop(0, GROUPS // 2, gather, tuple(blank for _ in range(8)))
    left = (sums[0] + sums[2]) + (sums[4] + sums[6])
    right = (sums[1] + sums[3]) + (sums[5] + sums[7])
    here_rows = pl.ds(pl.multiple_of(lat * ROWS, ROWS), ROWS)
    fields[2, here_rows, 0:LANES] = 4.0 * jnp.sqrt(left / SPEC)
    fields[2, here_rows, LANES:COLS] = 4.0 * jnp.sqrt(right / SPEC)
    fields[3, here_rows, 0:COLS] = own_sea[...].astype(f32)

    for step in range(1, LAT):
        peer = lax.rem(lat + step, LAT)
        part = fields.at[pl.ds(2, 2), here_rows, pl.ds(0, COLS)]
        pltpu.make_async_remote_copy(
            src_ref=part,
            dst_ref=part,
            send_sem=lat_sems.at[0],
            recv_sem=lat_sems.at[1],
            device_id=(peer, lon),
            device_id_type=MESH,
        ).start()

    send_west = pltpu.make_async_remote_copy(
        src_ref=own_edge,
        dst_ref=cols_east,
        send_sem=col_sems.at[0],
        recv_sem=col_sems.at[1],
        device_id=(lat, west),
        device_id_type=MESH,
    )
    send_east = pltpu.make_async_remote_copy(
        src_ref=own_edge,
        dst_ref=cols_west,
        send_sem=col_sems.at[2],
        recv_sem=col_sems.at[3],
        device_id=(lat, east),
        device_id_type=MESH,
    )
    send_west.start()
    send_east.start()

    pick_chunk(2)

    def forward(number, carry):
        pick_chunk(number)
        send_chunk(number - 1)
        return carry

    early = chunks * 5 // 11
    lax.fori_loop(3, early, forward, 0)

    @pl.when(lat == 0)
    def _():
        rows[0 : 2 * cap, :] = jnp.zeros((2 * cap, LANES), f32)

    @pl.when(lat == LAT - 1)
    def _():
        rows[2 * cap : 4 * cap, :] = jnp.zeros((2 * cap, LANES), f32)

    got = pl.ds(0, DEV - 1)
    pltpu.make_async_copy(inbox.at[got], inbox.at[got], box_sems.at[1]).wait()
    turned[...] = inbox[...].T

    def place(number, carry):
        base = pl.multiple_of(number * 8, 8)
        misfits = turned[pl.ds(base, 8), :]
        weights = turned[pl.ds(base + 32, 8), :]
        cell = turned[pl.ds(base + 64, 8), :].astype(i32)
        cell_row = lax.shift_right_logical(cell, 8)
        cell_col = lax.bitwise_and(cell, 255)
        rows8 = lax.broadcasted_iota(i32, (8, LANES), 0)
        cols = lax.broadcasted_iota(i32, (COLS, LANES), 0)
        spots, sent = [], []
        for s in range(8):
            spots.append(jnp.where(cols == cell_col[s : s + 1, :], 1.0, 0.0).astype(bf16))
            at_row = rows8 == cell_row[s : s + 1, :]
            sent.append(
                jnp.concatenate(
                    [
                        jnp.where(at_row, misfits[s : s + 1, :], 0.0),
                        jnp.where(at_row, weights[s : s + 1, :], 0.0),
                    ],
                    axis=0,
                )
            )
        spots = jnp.concatenate(spots, axis=1)
        sent = jnp.concatenate(sent, axis=1)
        total = lax.dot_general(
            jnp.concatenate(thirds(sent), axis=0), spots, NT, preferred_element_type=f32
        )
        total = total[0:16, :] + total[16:32, :] + total[32:48, :]
        fields[0, pl.ds(base, 8), 0:COLS] = total[0:8, :]
        fields[1, pl.ds(base, 8), 0:COLS] = total[8:16, :]
        return carry

    lax.fori_loop(0, LAT, place, 0)

    three = fields.at[pl.ds(2, 2), pl.ds(0, NROW - ROWS), pl.ds(0, COLS)]
    pltpu.make_async_copy(three, three, lat_sems.at[1]).wait()
    pltpu.make_async_copy(three, three, lat_sems.at[0]).wait()
    height = fields[2, :, 0:COLS]
    ocean = fields[3, :, 0:COLS]
    weight = fields[1, :, 0:COLS] * ocean
    fields[0, :, 0:COLS] = (fields[0, :, 0:COLS] - height * fields[1, :, 0:COLS]) * ocean
    fields[1, :, 0:COLS] = weight

    rim_west = pltpu.make_async_remote_copy(
        src_ref=fields.at[pl.ds(0, 4), pl.ds(0, NROW), pl.ds(0, LANES)],
        dst_ref=near_east,
        send_sem=rim_sems.at[0],
        recv_sem=rim_sems.at[1],
        device_id=(lat, west),
        device_id_type=MESH,
    )
    rim_east = pltpu.make_async_remote_copy(
        src_ref=fields.at[pl.ds(0, 4), pl.ds(0, NROW), pl.ds(LANES, LANES)],
        dst_ref=near_west,
        send_sem=rim_sems.at[2],
        recv_sem=rim_sems.at[3],
        device_id=(lat, east),
        device_id_type=MESH,
    )
    rim_west.start()
    rim_east.start()
    lax.fori_loop(early, chunks, forward, 0)
    send_chunk(chunks - 1)
    rim_west.wait()
    rim_east.wait()
    lane = lax.broadcasted_iota(i32, (NROW, LANES), 1)
    for number, filler in enumerate((0.0, 0.0, 1.0, 0.0)):
        fields[number, :, COLS:EXT] = jnp.where(
            lane < RIM,
            near_east[number],
            jnp.where(lane >= LANES - RIM, near_west[number], filler),
        )

    row = lax.broadcasted_iota(i32, (NROW, EXT), 0)

    def north_of(x):
        return jnp.where(row == NROW - 1, 0.0, pltpu.roll(x, NROW - 1, 0))

    def south_of(x):
        return jnp.where(row == 0, 0.0, pltpu.roll(x, 1, 0))

    def east_of(x):
        return pltpu.roll(x, EXT - 1, 1)

    def west_of(x):
        return pltpu.roll(x, 1, 1)

    ocean = fields[3]
    share = spread_rate * ocean
    keep = 1.0 - share * (
        north_of(ocean) + south_of(ocean) + east_of(ocean) + west_of(ocean)
    )

    def relax(x):
        return keep * x + share * (
            (north_of(x) + south_of(x)) + (east_of(x) + west_of(x))
        )

    def relax_both(_, pair):
        return relax(pair[0]), relax(pair[1])

    misfit, weight = lax.fori_loop(0, PASSES, relax_both, (fields[0], fields[1]))
    increment = ocean * misfit / (prior_weight + weight)
    factor = jnp.exp(2.0 * increment / fields[2]) * ocean
    going_up = factor * north_of(ocean)
    going_down = factor * south_of(ocean)
    for number, value in enumerate(
        (
            factor,
            factor * east_of(ocean),
            factor * west_of(ocean),
            going_up,
            going_down,
            south_of(going_up),
            north_of(going_down),
            increment,
        )
    ):
        padded[number] = value
    own = here_rows
    sub = lax.broadcasted_iota(i32, (ROWS, LANES), 0)
    for number in range(7):
        for half in range(2):
            value = padded[number, own, half * LANES : (half + 1) * LANES]
            if number == 5:
                rim_tables[8 * half : 8 * half + 8, :] = jnp.where(sub == 0, value, 0.0)
                value = jnp.where(sub == 0, 0.0, value)
            if number == 6:
                outer = sub == ROWS - 1
                rim_tables[16 + 8 * half : 24 + 8 * half, :] = jnp.where(
                    outer, value, 0.0
                )
                value = jnp.where(outer, 0.0, value)
            tables[16 * number + 8 * half : 16 * number + 8 * half + 8, :] = value
    increments[...] = padded[7, own, 0:COLS]
    beside = (
        jnp.broadcast_to(padded[1, own, EXT - 1 : EXT], (ROWS, LANES)),
        jnp.broadcast_to(padded[2, own, COLS : COLS + 1], (ROWS, LANES)),
    )

    send_west.wait()
    send_east.wait()

    def advance(step, carry):
        rims = cols_west[step] * beside[0], cols_east[step] * beside[1]
        for u in range(GROUP):
            at = 8 + (step * GROUP + u) * 16
            near = steps[2, step, u]
            speed = jnp.full((ROWS, LANES), speeds[step, u])
            back = speed < 0.0
            cell, flow = [], []
            for half in range(2):
                first = 8 * half
                cell.append(cells[pl.ds(pl.multiple_of(at + first, 8), 8), :])
                way = jnp.where(
                    back, tables[32 + first : 40 + first, :], tables[16 + first : 24 + first, :]
                )
                flow.append(cell[half] * way)
            shift = steps[0, step, u]
            moved = pltpu.roll(flow[0], shift, 1), pltpu.roll(flow[1], shift, 1)
            rim = pltpu.roll(jnp.where(back, rims[1], rims[0]), steps[1, step, u], 1)
            at_edge = lane == jnp.where(back, LANES - 1, 0)
            came = (
                jnp.where(at_edge, jnp.where(back, moved[1], rim), moved[0]),
                jnp.where(at_edge, jnp.where(back, rim, moved[0]), moved[1]),
            )
            speed = jnp.abs(speed)
            slow = jnp.full((ROWS, LANES), speeds[GROUPS + step, u])
            down = slow < 0.0
            slow = jnp.abs(slow)
            for half in range(2):
                first = 8 * half
                way = jnp.where(
                    down, tables[64 + first : 72 + first, :], tables[48 + first : 56 + first, :]
                )
                way_in = jnp.where(
                    down, tables[96 + first : 104 + first, :], tables[80 + first : 88 + first, :]
                )
                gone = cell[half] * way - cells[pl.ds(near + first, 8), :] * way_in
                to = pl.multiple_of((step * GROUP + u) * 16 + first, 8)
                partial[pl.ds(to, 8), :] = (
                    cell[half] * tables[first : first + 8, :]
                    - speed * (flow[half] - came[half])
                    - slow * gone
                )
        return carry

    lane = lax.broadcasted_iota(i32, (ROWS, LANES), 1)
    lax.fori_loop(0, GROUPS, advance, 0)

    pltpu.make_async_copy(inbox.at[got], inbox.at[got], box_sems.at[0]).wait()

    @pl.when(lat < LAT - 1)
    def _():
        north_copy(0, 2 * cap).wait_send()
        part = rows.at[pl.ds(2 * cap, 2 * cap)]
        pltpu.make_async_copy(part, part, row_sems.at[3]).wait()

    @pl.when(lat > 0)
    def _():
        south_copy(0, 2 * cap).wait_send()
        part = rows.at[pl.ds(0, 2 * cap)]
        pltpu.make_async_copy(part, part, row_sems.at[1]).wait()


def exchange(cap, spectrum, courant, *observed):
    vmem = pl.BlockSpec(memory_space=pltpu.VMEM)
    lists = -(-cap // LANES)
    return pl.pallas_call(
        functools.partial(exchange_kernel, cap),
        out_shape=(
            jax.ShapeDtypeStruct((CELLS, LANES), f32),
            jax.ShapeDtypeStruct((32, LANES), f32),
            jax.ShapeDtypeStruct((ROWS, COLS), f32),
            jax.ShapeDtypeStruct((4 * cap, LANES), f32),
            jax.ShapeDtypeStruct((GROUPS, GROUP), i32),
            jax.ShapeDtypeStruct((2 * GROUPS, GROUP), f32),
        ),
        in_specs=[pl.BlockSpec(memory_space=pl.ANY)] * 7,
        out_specs=(vmem,) * 6,
        scratch_shapes=[
            pltpu.VMEM((CELLS + 16, LANES), f32),
            pltpu.VMEM((112, LANES), f32),
            pltpu.VMEM((GROUPS, ROWS, LANES), f32),
            pltpu.VMEM((GROUPS, ROWS, LANES), f32),
            pltpu.VMEM((3, GROUPS, GROUP), i32),
            pltpu.SMEM((3, GROUPS, GROUP), i32),
            pltpu.SMEM((2 * GROUPS, GROUP), f32),
            pltpu.VMEM((2, SPEC), f32),
            pltpu.VMEM((1, 256), i32),
            pltpu.VMEM((1, 256), i32),
            pltpu.VMEM((1, 256), f32),
            pltpu.VMEM((1, 256), f32),
            pltpu.VMEM((ROWS, COLS), i32),
            pltpu.VMEM((LON, LANES), f32),
            pltpu.VMEM((DEV, LANES), f32),
            pltpu.VMEM((LANES, DEV), f32),
            pltpu.VMEM((4, NROW, EXT), f32),
            pltpu.VMEM((4, NROW, LANES), f32),
            pltpu.VMEM((4, NROW, LANES), f32),
            pltpu.VMEM((GROUPS, ROWS, LANES), f32),
            pltpu.VMEM((8, NROW, EXT), f32),
            pltpu.VMEM((2 * cap, LANES), f32),
            pltpu.VMEM((2 * cap, LANES), f32),
            pltpu.VMEM((2, lists, LANES), i32),
            pltpu.SMEM((2, lists, LANES), i32),
            pltpu.SemaphoreType.DMA((LOADS,)),
            pltpu.SemaphoreType.DMA((8,)),
            pltpu.SemaphoreType.DMA,
            pltpu.SemaphoreType.DMA((2,)),
            pltpu.SemaphoreType.DMA((2,)),
            pltpu.SemaphoreType.DMA((4,)),
            pltpu.SemaphoreType.DMA((4,)),
            pltpu.SemaphoreType.DMA((4,)),
        ],
        compiler_params=pltpu.CompilerParams(
            collective_id=0 if cap == CAP_HALF else 1,
            has_side_effects=True,
            vmem_limit_bytes=30 * 2**20,
        ),
        name=f"exchange_{cap}",
    )(spectrum, courant, *observed)


def update_kernel(
    partial,
    rim_tables,
    increments,
    rows,
    places,
    speeds,
    out,
    increment,
    stage,
    place,
    speed,
    sems,
    out_sems,
):
    copies = [
        pltpu.make_async_copy(places, place, sems.at[0]),
        pltpu.make_async_copy(speeds, speed, sems.at[1]),
    ]
    for copy in copies:
        copy.start()
    increment[...] = increments[...]
    for copy in copies:
        copy.wait()
    size = GROUP * 16

    def store(group):
        part = pl.ds(pl.multiple_of(group * size, size), size)
        return pltpu.make_async_copy(stage.at[part], out.at[part], out_sems.at[group])

    def finish(step):
        for u in range(GROUP):
            at = (step * GROUP + u) * 16
            slow = jnp.full((ROWS, LANES), speed[GROUPS + step, u])
            down = slow < 0.0
            slow = jnp.abs(slow)
            line = place[step, u]
            for half in range(2):
                first = 8 * half
                way = jnp.where(
                    down,
                    rim_tables[16 + first : 24 + first, :],
                    rim_tables[first : first + 8, :],
                )
                row = jnp.broadcast_to(rows[pl.ds(line + half, 1), :], (ROWS, LANES))
                here = pl.ds(pl.multiple_of(at + first, 8), 8)
                stage[here, :] = partial[here, :] + slow * (row * way)

    finish(0)

    def follow(step, carry):
        finish(step)
        store(step - 1).start()
        return carry

    lax.fori_loop(1, GROUPS, follow, 0)
    store(GROUPS - 1).start()
    lax.fori_loop(0, GROUPS, lambda g, carry: (store(g).wait(), carry)[1], 0)


def update(cap, *sent):
    vmem = pl.BlockSpec(memory_space=pltpu.VMEM)
    return pl.pallas_call(
        update_kernel,
        out_shape=(
            jax.ShapeDtypeStruct((CELLS, LANES), f32),
            jax.ShapeDtypeStruct((ROWS, COLS), f32),
        ),
        in_specs=[vmem] * 6,
        out_specs=(pl.BlockSpec(memory_space=pl.ANY), vmem),
        scratch_shapes=[
            pltpu.VMEM((CELLS, LANES), f32),
            pltpu.SMEM((GROUPS, GROUP), i32),
            pltpu.SMEM((2 * GROUPS, GROUP), f32),
            pltpu.SemaphoreType.DMA((2,)),
            pltpu.SemaphoreType.DMA((GROUPS,)),
        ],
        compiler_params=pltpu.CompilerParams(vmem_limit_bytes=20 * 2**20),
        name=f"update_{cap}",
    )(*sent)


def body(spectrum, sea_mask, courant, obs_tile, obs_cell, obs_value, obs_error):
    halves = spectrum.reshape(SPEC, ROWS, 2, LANES).transpose(0, 2, 1, 3)
    observed = (
        obs_tile.reshape(1, -1),
        obs_cell.reshape(1, -1),
        obs_value.reshape(1, -1),
        obs_error.reshape(1, -1),
        sea_mask,
    )
    over = jnp.sum((courant[1] < 0.0).astype(i32)) - (SPEC - CAP_HALF)
    fits = over.astype(jnp.uint32) <= 2 * CAP_HALF - SPEC

    def run(cap):
        sent = exchange(cap, halves.reshape(CELLS, LANES), courant, *observed)
        return update(cap, *sent)

    updated, increment = lax.cond(fits, lambda: run(CAP_HALF), lambda: run(CAP_ALL))
    updated = updated.reshape(SPEC, 2, ROWS, LANES).transpose(0, 2, 1, 3)
    return updated.reshape(SPEC, ROWS, COLS), increment


def solution(mesh):
    return jax.shard_map(
        body,
        mesh=mesh,
        in_specs=(
            P(None, "lat", "lon"),
            P("lat", "lon"),
            P(),
            P(("lat", "lon"), None),
            P(("lat", "lon")),
            P(("lat", "lon")),
            P(("lat", "lon")),
        ),
        out_specs=(P(None, "lat", "lon"), P("lat", "lon")),
        check_vma=False,
    )
```
